32 devices in a mesh: dp: 4 (over y, core), label: 8 (over z, x).
Axes of the slice: x: 2, y: 2, z: 4, core: 2. Of those that a mesh axis runs over, the one named last changes fastest.
Arguments:
- queries: bfloat16 [4096, 512], P(('dp', 'label')), may hold values from -200 to 200
- shortlist: int32 [4096, 4], P(('dp', 'label')), may hold values from 0 to 511, all different within a row; in each aligned block of 128 rows (0 to 127, 128 to 255, ...) at most 2 rows name the same one
- slab_slot: int32 [512], replicated, may hold values from 0 to 511, each once
- top_target: int32 [4096], P(('dp', 'label')), may hold values from 0 to 2047
- leaf_target: int32 [4096], P(('dp', 'label')), may hold values from 0 to 127
- top_weight: bfloat16 [2048, 512], P('label'), may hold values from -0.25 to 0.25
- mid_weight: bfloat16 [512, 512], P(('dp', 'label')), may hold values from -0.25 to 0.25
- leaf_weight: bfloat16 [512, 128, 512], P(('dp', 'label')), may hold values from -0.25 to 0.25
Outputs:
- query_grad: float32 [4096, 512], P(('dp', 'label'))
- top_grad: float32 [2048, 512], P('label')
- mid_grad: float32 [512, 512], P(('dp', 'label'))
- leaf_grad: float32 [512, 128, 512], P(('dp', 'label'))
- losses: float32 [3, 4096], P(None, ('dp', 'label'))
The draws below stay inside these ranges and needn't reach their ends.
Inputs may be any that keep to these rules, and one draw needn't show every extreme that they name: `shortlist`: each query names 4 different mid clusters; among the 128 queries of one device no cluster is named more than 2 times. Each cluster's mid and leaf rows are row slab_slot[c] of mid_weight and leaf_weight; every row is used once.
All inputs are finite; a program needn't handle non-finite values.
Results may differ from the reference program's by a relative error of at most 0.003.
Values may be sent and summed in bfloat16 or wider, within the bound.
No kernel may reach another device: no remote copies, remote signals or barrier semaphores. Data moves between devices by JAX's collectives and lax.ppermute only.
A program may use at most 64 MiB of HBM per device.

```python
import math
import jax
import jax.numpy as jnp
import numpy as np
from jax import lax

D = 512
TOPC = 2048
LEAF = 128
SHORT = 4
BLOCKS = 512
QD = 128
QTOT = 4096
CAPB = 2
DEVICES = 32


def draw_queries(key, part):
    values = jax.random.normal(key, (QTOT, D), jnp.float32)
    values = jnp.clip(values, -5.0, 5.0)
    return values.astype(jnp.bfloat16)


def touch_ends(drawn, own_key, smallest, largest):
    dims = drawn.shape
    place = [jax.random.randint(jax.random.fold_in(own_key, axis), (), 0, dims[axis]) for axis in range(len(dims))]
    drawn = drawn.at[tuple(place)].set(smallest)
    longest = dims.index(max(dims))
    place[longest] = (place[longest] + 1) % dims[longest]
    return drawn.at[tuple(place)].set(largest)


def block_scale(own_key, dims, cuts, low, high):
    level = 1.0
    for dim, parts in cuts:
        draws = jax.random.uniform(jax.random.fold_in(jax.random.fold_in(own_key, 6), dim), (parts,), jnp.float32, low / len(cuts), high / len(cuts))
        level = level * jnp.repeat(jnp.exp(draws), dims[dim] // parts).reshape((-1,) + (1,) * (len(dims) - 1 - dim))
    return level


def routed_block(rng, own, number, rows, count, top, most, skew):
    sequence = jax.random.permutation(rng, count)
    packed, common = portions_of(count, rows * top, most, skew, True), portions_of(count, rows * top, most, skew, False)
    places = jnp.arange(count)

    def named(tallies, rotation):
        used = int((tallies > 0).sum())
        fixed = max(1, used // 4)
        shifted = fixed + (places - fixed + rotation * (used - fixed)) % max(1, count - fixed)
        return jnp.zeros((count,), jnp.int32).at[sequence[jnp.where(places < fixed, places, shifted)]].set(jnp.asarray(tallies, jnp.int32))

    tallies = jnp.where(number % 4 == 0, named(packed, number // 4), named(common, number - number // 4 - 1))
    mixed = jax.random.permutation(jax.random.fold_in(own, 3), count)
    donor, sink = mixed[0:count // 2 * 2:2], mixed[1:count // 2 * 2:2]
    margin = jnp.minimum(tallies[donor] - 1, most - tallies[sink]) // 2
    margin = jnp.where((donor == sequence[0]) | (sink == sequence[0]) | (tallies[sink] == 0), 0, jnp.maximum(margin, 0))
    shifted = jax.random.randint(jax.random.fold_in(own, 4), (count // 2,), 0, 1 << 20) % (margin + 1)
    tallies = tallies.at[donor].add(-shifted).at[sink].add(shifted)
    items = jnp.searchsorted(jnp.cumsum(tallies), jnp.arange(rows * top), side="right").astype(jnp.int32)
    listing = items.reshape(top, rows).T
    listing = listing[jax.random.permutation(jax.random.fold_in(own, 1), rows)]
    rotation = jax.random.randint(jax.random.fold_in(own, 2), (rows, 1), 0, top)
    return jnp.take_along_axis(listing, (jnp.arange(top)[None, :] + rotation) % top, axis=1)


def portions_of(amount, total, most, skew, full):
    loads = [(1 << 20) // math.isqrt(rank ** skew) + 1 for rank in range(1, amount + 1)]
    largest = most if full else min(most, max(-(-total // amount), total * loads[0] // sum(loads)))
    least = 1 if total - largest >= amount - 1 else 0
    counts, rest = [largest] + [least] * (amount - 1), total - largest - least * (amount - 1)
    while rest > 0:
        free = [i for i in range(1, amount) if counts[i] < largest] or [i for i in range(1, amount) if counts[i] < most]
        mass, left = sum([loads[i] for i in free]), rest
        for i in free:
            addition = min(most - counts[i], max(1, left * loads[i] // mass), rest)
            counts[i] = counts[i] + addition
            rest = rest - addition
    return np.array(counts)


def normal_values(key, dims, scale, bound, cuts=(), kind=jnp.bfloat16):
    level = block_scale(key, dims, cuts, -0.22, 0.18) if cuts else 1.0
    values = jax.random.normal(key, dims, jnp.float32) * scale * level
    return jnp.minimum(jnp.maximum(values, -bound), bound).astype(kind)


def setup_inputs(seed: int = 0) -> dict:
    splits = jax.random.split(jax.random.key(seed), 9)
    queries = draw_queries(jax.random.fold_in(splits[8], 71), 0)
    shortlist_keys = jax.random.split(jax.random.fold_in(splits[1], 1), QTOT // QD)
    shortlist_turns = jax.random.permutation(jax.random.fold_in(splits[1], 3), QTOT // QD)
    shortlist = jax.vmap(lambda own, number: routed_block(jax.random.fold_in(splits[1], 2), own, number, QD, BLOCKS, SHORT, CAPB, 2))(shortlist_keys, shortlist_turns).reshape((QTOT, SHORT))
    slab_slot = jax.random.permutation(splits[2], BLOCKS).astype(jnp.int32)
    top_target = touch_ends(jax.random.randint(splits[3], (QTOT,), 0, TOPC), jax.random.fold_in(splits[3], 1), 0, TOPC - 1).astype(jnp.int32)
    leaf_target = touch_ends(jax.random.randint(splits[4], (QTOT,), 0, LEAF), jax.random.fold_in(splits[4], 1), 0, LEAF - 1).astype(jnp.int32)
    top_weight = normal_values(splits[5], (TOPC, D), D ** -0.5, 0.25, ((0, 8),))
    mid_weight = normal_values(splits[6], (BLOCKS, D), D ** -0.5, 0.25, ((0, 32),))
    leaf_weight = normal_values(splits[7], (BLOCKS, LEAF, D), D ** -0.5, 0.25, ((0, 32),))
    return dict(queries=queries, shortlist=shortlist, slab_slot=slab_slot, top_target=top_target, leaf_target=leaf_target, top_weight=top_weight, mid_weight=mid_weight, leaf_weight=leaf_weight)


def top_level(queries, top_target, top_weight):
    step_rows = QD * 8
    steps_count = queries.shape[0] // step_rows
    query_blocks = queries.reshape(steps_count, step_rows, D)
    target_blocks = top_target.reshape(steps_count, step_rows)
    columns = jnp.arange(TOPC, dtype=jnp.int32)

    def visit_block(accumulator, pieces):
        row_block, targets = pieces
        scores = jnp.dot(row_block, top_weight.T, preferred_element_type=jnp.float32)
        totals = jax.nn.logsumexp(scores, axis=1)
        target_hit = targets[:, None] == columns[None, :]
        top_loss = totals - jnp.sum(jnp.where(target_hit, scores, jnp.zeros_like(scores)), axis=1)
        dscore = (jnp.exp(scores - totals[:, None]) - target_hit.astype(jnp.float32)).astype(jnp.bfloat16)
        accumulator = accumulator + jnp.dot(dscore.T, row_block, preferred_element_type=jnp.float32)
        top_back = jnp.dot(dscore, top_weight, preferred_element_type=jnp.float32)
        return accumulator, (top_loss, top_back)

    start_grad = jnp.zeros((TOPC, D), jnp.float32)
    top_grad, (top_loss, top_back) = lax.scan(visit_block, start_grad, (query_blocks, target_blocks))
    return top_grad, top_loss.reshape(-1), top_back.reshape(-1, D)


def build_table(shortlist, slab_slot):
    position = slab_slot[shortlist].reshape(-1).astype(jnp.int32)
    sort_order = jnp.argsort(position, stable=True).astype(jnp.int32)
    ranked = position[sort_order]
    run_start = jnp.searchsorted(ranked, ranked, side="left").astype(jnp.int32)
    slot_rank = jnp.arange(ranked.shape[0], dtype=jnp.int32) - run_start
    pair_table = jnp.full((BLOCKS, DEVICES * CAPB), QTOT * SHORT, jnp.int32)
    return pair_table.at[ranked, slot_rank].set(sort_order)


def group_inputs(queries, pair_table, mid_weight, leaf_weight, group_index):
    padded = jnp.concatenate([queries, jnp.zeros((1, D), queries.dtype)], axis=0)
    group_table = lax.dynamic_slice_in_dim(pair_table, group_index * 16, 16, 0)
    query_index = (group_table // SHORT).astype(jnp.int32)
    row_block = padded[query_index].astype(jnp.float32)
    leaf_rows = lax.dynamic_slice_in_dim(leaf_weight, group_index * 16, 16, 0).astype(jnp.float32)
    mid_rows = lax.dynamic_slice_in_dim(mid_weight, group_index * 16, 16, 0).astype(jnp.float32)
    return group_table, query_index, row_block, leaf_rows, mid_rows


def leaf_forward(queries, pair_table, pair_codes, mid_weight, leaf_weight):
    codes_ext = jnp.concatenate([pair_codes, jnp.full((1,), -2, jnp.int32)])
    labels = jnp.arange(LEAF, dtype=jnp.int32)

    def visit_group(group_index):
        group_table, query_index, row_block, leaf_rows, mid_rows = group_inputs(queries, pair_table, mid_weight, leaf_weight, group_index)
        scores = jnp.einsum("gsd,gld->gsl", row_block, leaf_rows)
        mid_scores = jnp.einsum("gsd,gd->gs", row_block, mid_rows)
        block_lse = jax.nn.logsumexp(scores, axis=-1)
        target_hit = codes_ext[group_table][..., None] == labels
        target = jnp.sum(jnp.where(target_hit, scores, jnp.zeros_like(scores)), axis=-1)
        return mid_scores, block_lse, target

    outputs = lax.map(visit_group, jnp.arange(BLOCKS // 16, dtype=jnp.int32))
    flat_index = pair_table.reshape(-1)
    results = []
    for values in outputs:
        placed = jnp.zeros((QTOT * SHORT + 1,), jnp.float32).at[flat_index].set(values.reshape(-1))
        results.append(placed[:-1].reshape(QTOT, SHORT))
    return results[0], results[1], results[2]


def leaf_backward(queries, pair_table, pair_codes, pair_delta, pair_lse, mid_weight, leaf_weight):
    codes_ext = jnp.concatenate([pair_codes, jnp.full((1,), -2, jnp.int32)])
    delta_ext = jnp.concatenate([pair_delta, jnp.zeros((1,), pair_delta.dtype)])
    lse_ext = jnp.concatenate([pair_lse, jnp.zeros((1,), jnp.float32)])
    labels = jnp.arange(LEAF, dtype=jnp.int32)

    def visit_group(accumulator, group_index):
        group_table, query_index, row_block, leaf_rows, mid_rows = group_inputs(queries, pair_table, mid_weight, leaf_weight, group_index)
        scores = jnp.einsum("gsd,gld->gsl", row_block, leaf_rows)
        group_codes = codes_ext[group_table]
        live_slot = group_codes >= -1
        target_hit = (group_codes[..., None] == labels).astype(jnp.float32)
        slot_lse = lse_ext[group_table]
        leaf_delta = jnp.where(live_slot[..., None], jnp.exp(scores - slot_lse[..., None]) - target_hit, jnp.zeros_like(scores)).astype(jnp.bfloat16)
        leaf_float = leaf_delta.astype(jnp.float32)
        mid_float = delta_ext[group_table].astype(jnp.float32)
        leaf_part = jnp.einsum("gsl,gsd->gld", leaf_float, row_block)
        mid_part = jnp.einsum("gs,gsd->gd", mid_float, row_block)
        pair_back = (jnp.einsum("gsl,gld->gsd", leaf_float, leaf_rows) + mid_float[..., None] * mid_rows[:, None, :]).astype(jnp.bfloat16)
        accumulator = accumulator.at[query_index.reshape(-1)].add(pair_back.reshape(-1, D).astype(jnp.float32))
        return accumulator, (mid_part, leaf_part)

    start_sum = jnp.zeros((QTOT + 1, D), jnp.float32)
    summed, (mid_grad, leaf_grad) = lax.scan(visit_group, start_sum, jnp.arange(BLOCKS // 16, dtype=jnp.int32))
    return summed[:-1], mid_grad.reshape(BLOCKS, D), leaf_grad.reshape(BLOCKS, LEAF, D)


def reference(queries, shortlist, slab_slot, top_target, leaf_target, top_weight, mid_weight, leaf_weight):
    top_grad, top_loss, top_back = top_level(queries, top_target, top_weight)
    pair_table = build_table(shortlist, slab_slot)
    first_slot = (jnp.arange(SHORT, dtype=jnp.int32) == 0)[None, :]
    pair_codes = jnp.where(first_slot, leaf_target[:, None], -1).astype(jnp.int32).reshape(-1)
    mid_scores, block_lse, target = leaf_forward(queries, pair_table, pair_codes, mid_weight, leaf_weight)
    mid_totals = jax.nn.logsumexp(mid_scores, axis=1)
    mid_loss = mid_totals - mid_scores[:, 0]
    mid_delta = (jnp.exp(mid_scores - mid_totals[:, None]) - first_slot.astype(jnp.float32)).astype(jnp.bfloat16)
    leaf_lse = jax.nn.logsumexp(block_lse, axis=1)
    leaf_loss = leaf_lse - target[:, 0]
    pair_lse = jnp.broadcast_to(leaf_lse[:, None], (QTOT, SHORT)).reshape(-1)
    summed, mid_grad, leaf_grad = leaf_backward(queries, pair_table, pair_codes, mid_delta.reshape(-1), pair_lse, mid_weight, leaf_weight)
    query_grad = top_back + summed
    losses = jnp.stack([top_loss, mid_loss, leaf_loss])
    return query_grad, top_grad, mid_grad, leaf_grad, losses
```

```python
import functools

import jax
import jax.numpy as jnp
from jax import lax
from jax.experimental import pallas as pl
from jax.experimental.pallas import tpu as pltpu
from jax.sharding import PartitionSpec as P

D = 512
BLOCKS = 512
CAPB = 2


def shortened(array):

    def short(part):
        return part.astype(jnp.bfloat16) if part.dtype == jnp.float32 else part

    return jax.tree.map(short, array)


def route_narrow(payload):
    return jax.tree.map(
        lambda part, own: part.astype(own.dtype),
        lax.all_to_all(
            lax.all_to_all(shortened(payload), "label", split_axis=1, concat_axis=1, tiled=True),
            "dp",
            split_axis=0,
            concat_axis=0,
            tiled=True,
        ),
        payload,
    )


def route_wide(payload):
    return lax.all_to_all(
        lax.all_to_all(payload, "label", split_axis=1, concat_axis=1, tiled=True),
        "dp",
        split_axis=0,
        concat_axis=0,
        tiled=True,
    )


def per_device_any(
    queries, shortlist, slab_slot, top_target, leaf_target, top_weight, mid_weight, leaf_weight
):
    dp_size = lax.axis_size("dp")
    label_size = lax.axis_size("label")
    rows_here = queries.shape[0]
    short_len = shortlist.shape[1]
    block_dev = leaf_weight.shape[0]
    all_rows = lax.all_gather(top_weight, "label", axis=0, tiled=True)
    scores = jnp.dot(queries, all_rows.T, preferred_element_type=jnp.float32)
    totals = jax.nn.logsumexp(scores, axis=1)
    target_hit = top_target[:, None] == jnp.arange(scores.shape[1], dtype=jnp.int32)[None, :]
    top_loss = totals - jnp.sum(jnp.where(target_hit, scores, 0.0), axis=1)
    dscore = (jnp.exp(scores - totals[:, None]) - target_hit.astype(jnp.float32)).astype(
        jnp.bfloat16
    )
    top_back = jnp.dot(dscore, all_rows, preferred_element_type=jnp.float32)
    columns_held = lax.all_to_all(dscore, "label", split_axis=1, concat_axis=0, tiled=True)
    top_part = lax.dot_general(
        columns_held,
        lax.all_gather(queries, "label", axis=0, tiled=True),
        (((0,), (0,)), ((), ())),
        preferred_element_type=jnp.float32,
    )
    top_grad = lax.psum(top_part, "dp")
    position = slab_slot[shortlist].reshape(-1)
    sort_order = jnp.argsort(position, stable=True)
    ranked = position[sort_order]
    run_start = jnp.searchsorted(ranked, ranked, side="left")
    slot_rank = jnp.arange(ranked.shape[0], dtype=jnp.int32) - run_start
    slot_of = jnp.zeros_like(position).at[sort_order].set(ranked * CAPB + slot_rank)
    first_slot = (jnp.arange(short_len, dtype=jnp.int32) == 0)[None, :]
    pair_codes = jnp.where(first_slot, leaf_target[:, None], -1).reshape(-1).astype(jnp.float32)
    layout = (dp_size, label_size, block_dev, CAPB)
    send_rows = (
        jnp.zeros((BLOCKS * CAPB, D), jnp.bfloat16)
        .at[slot_of]
        .set(jnp.repeat(queries, short_len, axis=0))
    )
    send_code = (
        jnp.full((BLOCKS * CAPB,), -2.0, jnp.float32)
        .at[slot_of]
        .set(pair_codes)
        .astype(jnp.bfloat16)
    )
    got_rows, got_code = route_narrow((send_rows.reshape(layout + (D,)), send_code.reshape(layout)))
    scores_held = jnp.einsum(
        "abkcd,kld->abkcl", got_rows, leaf_weight, preferred_element_type=jnp.float32
    )
    mid_held = jnp.einsum(
        "abkcd,kd->abkc", got_rows, mid_weight, preferred_element_type=jnp.float32
    )
    block_lse = jax.nn.logsumexp(scores_held, axis=-1)
    code_float = got_code.astype(jnp.float32)
    labels = jnp.arange(scores_held.shape[-1], dtype=jnp.float32)
    target_hit = (code_float[..., None] == labels).astype(jnp.float32)
    target_held = jnp.sum(scores_held * target_hit, axis=-1)
    back_mid, back_lse, back_target = route_wide((mid_held, block_lse, target_held))
    pair_mid = back_mid.reshape(-1)[slot_of].reshape(rows_here, short_len)
    pair_lse = back_lse.reshape(-1)[slot_of].reshape(rows_here, short_len)
    pair_target = back_target.reshape(-1)[slot_of].reshape(rows_here, short_len)
    mid_totals = jax.nn.logsumexp(pair_mid, axis=1)
    mid_loss = mid_totals - pair_mid[:, 0]
    mid_delta = (jnp.exp(pair_mid - mid_totals[:, None]) - first_slot.astype(jnp.float32)).astype(
        jnp.bfloat16
    )
    leaf_lse = jax.nn.logsumexp(pair_lse, axis=1)
    leaf_loss = leaf_lse - pair_target[:, 0]
    send_delta = (
        jnp.zeros((BLOCKS * CAPB,), jnp.float32)
        .at[slot_of]
        .set(mid_delta.reshape(-1).astype(jnp.float32))
    )
    send_lse = (
        jnp.zeros((BLOCKS * CAPB,), jnp.float32).at[slot_of].set(jnp.repeat(leaf_lse, short_len))
    )
    got_delta, got_lse = route_wide((send_delta.reshape(layout), send_lse.reshape(layout)))
    live_slot = code_float > -1.5
    leaf_delta = jnp.where(
        live_slot[..., None], jnp.exp(scores_held - got_lse[..., None]) - target_hit, 0.0
    ).astype(jnp.bfloat16)
    mid_slots = got_delta.astype(jnp.bfloat16)
    leaf_grad = jnp.einsum(
        "abkcl,abkcd->kld", leaf_delta, got_rows, preferred_element_type=jnp.float32
    )
    mid_grad = jnp.einsum("abkc,abkcd->kd", mid_slots, got_rows, preferred_element_type=jnp.float32)
    pair_back = jnp.einsum(
        "abkcl,kld->abkcd", leaf_delta, leaf_weight, preferred_element_type=jnp.float32
    )
    pair_back = (
        pair_back
        + mid_slots.astype(jnp.float32)[..., None] * mid_weight.astype(jnp.float32)[:, None, :]
    ).astype(jnp.bfloat16)
    returned = route_narrow(pair_back)
    pair_sum = (
        returned.reshape(BLOCKS * CAPB, D)[slot_of]
        .astype(jnp.float32)
        .reshape(rows_here, short_len, D)
        .sum(axis=1)
    )
    query_grad = top_back + pair_sum
    losses = jnp.stack([top_loss, mid_loss, leaf_loss])
    return (query_grad, top_grad, mid_grad, leaf_grad, losses)


LANES = 128
SUB = 8
BF = jnp.bfloat16
F32 = jnp.float32
HIGH = lax.Precision.HIGHEST


def params():
    return pltpu.CompilerParams(vmem_limit_bytes=56 * 1024 * 1024)


def iota(shape, dim):
    return lax.broadcasted_iota(jnp.int32, shape, dim)


def iota_f(shape, dim):
    return iota(shape, dim).astype(F32)


def dot_nn(a, b, precision=None):
    return lax.dot_general(
        a, b, (((1,), (0,)), ((), ())), precision=precision, preferred_element_type=F32
    )


def dot_nt(a, b, precision=None):
    return lax.dot_general(
        a, b, (((1,), (1,)), ((), ())), precision=precision, preferred_element_type=F32
    )


def dot_tn(a, b, precision=None):
    return lax.dot_general(
        a, b, (((0,), (0,)), ((), ())), precision=precision, preferred_element_type=F32
    )


def pack_kernel(q_ref, short_ref, slab_ref, leaf_t_ref, pay_ref, info_ref, *, devs, held):
    rows, width = q_ref.shape
    short_len = short_ref.shape[1]
    clusters = slab_ref.shape[1]
    chunks = width // LANES
    slots = CAPB * held
    cluster_f = iota_f((rows, clusters), 1)
    slab = jnp.broadcast_to(slab_ref[...].astype(F32), (rows, clusters))
    short = short_ref[...].astype(F32)
    places, hits = [], []
    for j in range(short_len):
        place = jnp.sum(jnp.where(short[:, j : j + 1] == cluster_f, slab, 0.0), axis=1, keepdims=True)
        places.append(place)
        hits.append(jnp.where(place == cluster_f, 1.0, 0.0))
    hit = functools.reduce(lambda a, b: a + b, hits)
    before = jnp.where(iota((rows, rows), 1) < iota((rows, rows), 0), 1.0, 0.0).astype(BF)
    count = dot_nn(before, hit.astype(BF))
    lane = iota((rows, LANES), 1)
    info = jnp.zeros((rows, LANES), F32)
    for j in range(short_len):
        rank = jnp.sum(hits[j] * count, axis=1, keepdims=True)
        info = jnp.where(lane == j, places[j], info)
        info = jnp.where(lane == short_len + j, rank, info)
    info_ref[...] = info
    queries = q_ref[...]
    target = jnp.broadcast_to(leaf_t_ref[...].astype(F32) + 1.0, (SUB, rows)).astype(BF)
    ones = jnp.ones((SUB, rows), BF)
    table_rows = clusters // LANES
    table = jnp.zeros((CAPB * table_rows, LANES), F32)
    sub = iota((CAPB * table_rows, LANES), 0)
    for r in range(CAPB):
        pick = jnp.where(count == float(r), hit, 0.0)
        chosen = pick.astype(BF)
        first = (pick * hits[0]).astype(BF)
        code = dot_nn(ones, chosen) + dot_nn(target, first)
        for i in range(table_rows):
            part = jnp.broadcast_to(code[0:1, i * LANES : (i + 1) * LANES], table.shape)
            table = jnp.where(sub == r * table_rows + i, part, table)
        got = dot_tn(chosen, queries).astype(BF)
        for c in range(chunks):
            start = c * slots + r * held
            pay_ref[:, start : start + held, :] = got[:, c * LANES : (c + 1) * LANES].reshape(
                devs, held, LANES
            )
    coded = table.astype(BF)
    pay_ref[:, chunks * slots :, :] = jnp.broadcast_to(coded[None], (devs,) + coded.shape)


def forward_kernel(
    place_ref, got_ref, leaf_ref, mid_ref, rows_ref, score_ref, code_ref, stat_ref, wide_ref, table_ref
):
    devs, depth, _ = got_ref.shape
    held, labels, width = leaf_ref.shape
    chunks = width // LANES
    slots = CAPB * held
    body = chunks * slots
    wide_ref[...] = got_ref[:, :body, :].reshape(devs * body, LANES).astype(F32)
    tail = depth - body
    table_ref[...] = got_ref[:, body:, :].astype(F32).reshape(devs * tail, LANES)
    lane = iota((devs, LANES), 1)
    codes = jnp.zeros((devs, LANES), F32)
    for r in range(CAPB):
        row = table_ref[pl.ds(r * (tail // CAPB) + place_ref[0], devs, stride=tail), :]
        row = pltpu.roll(row, place_ref[1 + r], 1)
        codes = jnp.where((lane >= r * held) & (lane < (r + 1) * held), row, codes)
    code_ref[...] = codes
    label_f = iota_f((CAPB * devs, labels), 1)
    stats = jnp.zeros((devs, LANES), F32)
    for k in range(held):
        parts = []
        for r in range(CAPB):
            parts.append(
                jnp.concatenate(
                    [
                        wide_ref[pl.ds(c * slots + r * held + k, devs, stride=body), :]
                        for c in range(chunks)
                    ],
                    axis=1,
                )
            )
        full = jnp.concatenate(parts, axis=0)
        rows = full.astype(BF)
        rows_ref[k] = rows
        scores = dot_nt(rows, leaf_ref[k])
        score_ref[k] = scores
        mid = jnp.sum(full * mid_ref[k : k + 1, :].astype(F32), axis=1, keepdims=True)
        peak = jnp.max(scores, axis=1, keepdims=True)
        lse = peak + jnp.log(jnp.sum(jnp.exp(scores - peak), axis=1, keepdims=True))
        code = jnp.concatenate(
            [codes[:, r * held + k : r * held + k + 1] for r in range(CAPB)], axis=0
        )
        target = jnp.sum(jnp.where(code - 2.0 == label_f, scores, 0.0), axis=1, keepdims=True)
        for n, value in enumerate((mid, lse, target)):
            for r in range(CAPB):
                stats = jnp.where(
                    lane == n * slots + r * held + k, value[r * devs : (r + 1) * devs], stats
                )
    stat_ref[pl.ds(0, devs, stride=SUB), :] = stats


def middle_kernel(info_ref, stat_ref, out_ref, loss_ref, *, devs, held, short_len):
    rows = info_ref.shape[0]
    slots = CAPB * held
    info = info_ref[...]
    stats = stat_ref[pl.ds(0, devs, stride=SUB), :]
    lane = iota_f((rows, LANES), 1)
    dev_f = iota_f((rows, devs), 1)
    owners, spots, mids, lses = [], [], [], []
    for j in range(short_len):
        place = info[:, j : j + 1]
        rank = info[:, short_len + j : short_len + j + 1]
        dev = jnp.floor(place * (1.0 / held))
        spot = place - dev * held + rank * held
        owner = jnp.where(dev == dev_f, 1.0, 0.0)
        values = dot_nn(owner, stats, HIGH)
        owners.append(owner)
        spots.append(spot)
        mids.append(jnp.sum(jnp.where(lane == spot, values, 0.0), axis=1, keepdims=True))
        lses.append(jnp.sum(jnp.where(lane == spot + slots, values, 0.0), axis=1, keepdims=True))
        if j == 0:
            target = jnp.sum(
                jnp.where(lane == spot + 2 * slots, values, 0.0), axis=1, keepdims=True
            )

    def total(columns):
        peak = functools.reduce(jnp.maximum, columns)
        return peak + jnp.log(functools.reduce(lambda a, b: a + b, [jnp.exp(v - peak) for v in columns]))

    mid_total = total(mids)
    leaf_total = total(lses)
    back = []
    for j in range(short_len):
        delta = jnp.exp(mids[j] - mid_total) - (1.0 if j == 0 else 0.0)
        delta = delta.astype(BF).astype(F32)
        back.append(
            jnp.where(
                lane == spots[j], leaf_total, jnp.where(lane == spots[j] + slots, delta, 0.0)
            )
        )
    sent = dot_tn(jnp.concatenate(owners, axis=0), jnp.concatenate(back, axis=0), HIGH)
    out_ref[pl.ds(0, devs, stride=SUB), :] = sent
    losses = jnp.where(lane == 0.0, mid_total - mids[0], jnp.where(lane == 1.0, leaf_total - target, 0.0))
    loss_ref[...] = losses.T[:SUB, :]


def backward_kernel(
    score_ref, code_ref, norm_ref, leaf_ref, mid_ref, delta_ref, midcol_ref, pay_ref, wide_ref
):
    held, pairs, labels = score_ref.shape
    devs = pairs // CAPB
    width = leaf_ref.shape[2]
    chunks = width // LANES
    slots = CAPB * held
    body = chunks * slots
    norms = norm_ref[pl.ds(0, devs, stride=SUB), :]
    midcol_ref[...] = norms
    codes = code_ref[...]
    label_f = iota_f((pairs, labels), 1)

    def column(array, base, k):
        return jnp.concatenate(
            [array[:, base + r * held + k : base + r * held + k + 1] for r in range(CAPB)], axis=0
        )

    for k in range(held):
        code = column(codes, 0, k)
        lse = column(norms, 0, k)
        mid_delta = column(norms, slots, k)
        onehot = jnp.where(code - 2.0 == label_f, 1.0, 0.0)
        delta = jnp.where(code > 0.5, jnp.exp(score_ref[k] - lse) - onehot, 0.0).astype(BF)
        delta_ref[k] = delta
        back = dot_nn(delta, leaf_ref[k]) + mid_delta * mid_ref[k : k + 1, :].astype(F32)
        for r in range(CAPB):
            for c in range(chunks):
                wide_ref[pl.ds(c * slots + r * held + k, devs, stride=body), :] = back[
                    r * devs : (r + 1) * devs, c * LANES : (c + 1) * LANES
                ]
    pay_ref[...] = wide_ref[...].astype(BF).reshape(devs, body, LANES)


def grads_kernel(delta_ref, midcol_ref, rows_ref, leaf_grad_ref, mid_grad_ref):
    held, pairs, _ = delta_ref.shape
    devs = pairs // CAPB
    slots = CAPB * held
    norms = midcol_ref[...]
    for k in range(held):
        rows = rows_ref[k]
        leaf_grad_ref[k] = dot_tn(delta_ref[k], rows)
        mid_delta = jnp.concatenate(
            [norms[:, slots + r * held + k : slots + r * held + k + 1] for r in range(CAPB)], axis=0
        )
        mid_grad_ref[k : k + 1, :] = jnp.sum(mid_delta * rows.astype(F32), axis=0, keepdims=True)


def finish_kernel(info_ref, back_ref, top_ref, out_ref, *, held, short_len):
    rows, width = out_ref.shape
    devs = back_ref.shape[0]
    clusters = devs * held
    chunks = width // LANES
    slots = CAPB * held
    info = info_ref[...]
    cluster_f = iota_f((rows, clusters), 1)
    picks = []
    for r in range(CAPB):
        pick = jnp.zeros((rows, clusters), F32)
        for j in range(short_len):
            place = jnp.where(
                info[:, short_len + j : short_len + j + 1] == float(r), info[:, j : j + 1], -1.0
            )
            pick = jnp.where(place == cluster_f, 1.0, pick)
        picks.append(pick.astype(BF))
    for c in range(chunks):
        total = top_ref[:, c * LANES : (c + 1) * LANES]
        for r in range(CAPB):
            start = c * slots + r * held
            total = total + dot_nn(
                picks[r], back_ref[:, start : start + held, :].reshape(clusters, LANES)
            )
        out_ref[:, c * LANES : (c + 1) * LANES] = total


def top_kernel(
    where_ref, mine_ref, other_ref, wy_ref, wc_ref, own_ref, weight_ref,
    back_ref, part_ref, loss_ref, all_ref, *, rows, quarter,
):
    steps, depth, width = mine_ref.shape
    piece = 2 * steps * quarter
    for n in range(steps):
        all_ref[n * quarter : (n + 1) * quarter, :] = mine_ref[n, rows : rows + quarter, :]
        all_ref[(steps + n) * quarter : (steps + n + 1) * quarter, :] = other_ref[n, rows : rows + quarter, :]
    all_ref[piece : 2 * piece, :] = wy_ref[...]
    all_ref[2 * piece :, :] = wc_ref[...]
    held = weight_ref.shape[0]
    part_ref[...] = jnp.zeros(part_ref.shape, F32)
    held_base = where_ref[0].astype(F32)
    held_f = iota_f((rows, held), 1) + held_base
    for side, ref in ((0, mine_ref), (1, other_ref)):
        for n in range(steps):
            block = ref[n, :rows, :]
            scores = dot_nt(block, all_ref[...])
            peak = jnp.max(scores, axis=1, keepdims=True)
            total = peak + jnp.log(jnp.sum(jnp.exp(scores - peak), axis=1, keepdims=True))
            codes = ref[n, rows + quarter : rows + quarter + 16, :LANES].astype(F32)
            target = (codes[0:1, :] * 256.0 + codes[1:2, :])
            target = jnp.broadcast_to(target, (LANES, LANES)).T[:, 0:1]
            mine = dot_nt(block, weight_ref[...])
            delta = (jnp.exp(mine - total) - jnp.where(target == held_f, 1.0, 0.0)).astype(BF)
            part_ref[...] += dot_tn(delta, block)
            if side == 0 and n == 0:
                column = own_ref[...]
                hit = jnp.broadcast_to(column, scores.shape) == target
                full = (jnp.exp(scores - total) - jnp.where(hit, 1.0, 0.0)).astype(BF)
                back_ref[...] = dot_nn(full, all_ref[...])
                loss = total - jnp.sum(jnp.where(hit, scores, 0.0), axis=1, keepdims=True)
                loss_ref[...] = jnp.broadcast_to(loss, (rows, LANES)).T[:SUB, :]


def spec():
    return pl.BlockSpec(memory_space=pltpu.VMEM)


def call(kernel, outs, ins, scratch=(), scalars=0, name=None):
    return pl.pallas_call(
        kernel,
        out_shape=outs,
        in_specs=[pl.BlockSpec(memory_space=pltpu.SMEM)] * scalars + [spec()] * (len(ins) - scalars),
        out_specs=jax.tree.map(lambda _: spec(), outs),
        scratch_shapes=list(scratch),
        compiler_params=params(),
        name=name,
    )(*ins)


def shape(dims, dtype):
    return jax.ShapeDtypeStruct(dims, dtype)


def fits(queries, leaf_weight, shortlist, top_weight, devs, dp_size, label_size):
    rows, width = queries.shape
    held, labels = leaf_weight.shape[:2]
    return (
        rows == LANES
        and labels == LANES
        and width % LANES == 0
        and held % 16 == 0
        and LANES % held == 0
        and 3 * CAPB * held <= LANES
        and CAPB * (devs * held // LANES) % SUB == 0
        and devs % SUB == 0
        and dp_size == 4
        and label_size == 8
        and top_weight.shape[0] % (dp_size * 16) == 0
        and top_weight.shape[0] * label_size <= 65536
        and 2 * shortlist.shape[1] <= LANES
    )


def exchange(array):
    return lax.all_to_all(array, ("dp", "label"), split_axis=0, concat_axis=0, tiled=True)


def per_device(
    queries, shortlist, slab_slot, top_target, leaf_target, top_weight, mid_weight, leaf_weight
):
    dp_size = lax.axis_size("dp")
    label_size = lax.axis_size("label")
    devs = dp_size * label_size
    if not fits(queries, leaf_weight, shortlist, top_weight, devs, dp_size, label_size):
        return per_device_any(
            queries, shortlist, slab_slot, top_target, leaf_target, top_weight, mid_weight, leaf_weight
        )
    rows, width = queries.shape
    held, labels = leaf_weight.shape[:2]
    short_len = shortlist.shape[1]
    clusters = devs * held
    chunks = width // LANES
    slots = CAPB * held
    body = chunks * slots
    tail = CAPB * clusters // LANES
    dp_at = lax.axis_index("dp")
    label_at = lax.axis_index("label")
    me = dp_at * label_size + label_at

    payload, info = call(
        functools.partial(pack_kernel, devs=devs, held=held),
        (shape((devs, body + tail, LANES), BF), shape((rows, LANES), F32)),
        (queries, shortlist, slab_slot[None, :], leaf_target[None, :]),
        name="pack",
    )
    got = exchange(payload)
    first_place = me * held
    lane_at = first_place % LANES
    place = jnp.stack(
        [first_place // LANES] + [(r * held - lane_at) % LANES for r in range(CAPB)]
    ).astype(jnp.int32)
    rows_held, scores, codes, stats = call(
        forward_kernel,
        (
            shape((held, CAPB * devs, width), BF),
            shape((held, CAPB * devs, labels), F32),
            shape((devs, LANES), F32),
            shape((devs * SUB, LANES), F32),
        ),
        (place, got, leaf_weight, mid_weight),
        scratch=(pltpu.VMEM((devs * body, LANES), F32), pltpu.VMEM((devs * tail, LANES), F32)),
        scalars=1,
        name="forward",
    )
    stats_back = exchange(stats.reshape(devs, SUB, LANES)).reshape(devs * SUB, LANES)
    norms, pair_losses = call(
        functools.partial(middle_kernel, devs=devs, held=held, short_len=short_len),
        (shape((devs * SUB, LANES), F32), shape((SUB, rows), F32)),
        (info, stats_back),
        name="middle",
    )
    norms_held = exchange(norms.reshape(devs, SUB, LANES)).reshape(devs * SUB, LANES)
    delta, mid_cols, back = call(
        backward_kernel,
        (
            shape((held, CAPB * devs, labels), BF),
            shape((devs, LANES), F32),
            shape((devs, body, LANES), BF),
        ),
        (scores, codes, norms_held, leaf_weight, mid_weight),
        scratch=(pltpu.VMEM((devs * body, LANES), F32),),
        name="backward",
    )
    returned = exchange(back)
    leaf_grad, mid_grad = call(
        grads_kernel,
        (shape((held, labels, width), F32), shape((held, width), F32)),
        (delta, mid_cols, rows_held),
        name="grads",
    )

    steps = label_size // 2
    quarter = top_weight.shape[0] // dp_size
    held_top = top_weight.shape[0]
    codes_top = jnp.zeros((16, width), BF)
    codes_top = codes_top.at[0, :rows].set((top_target // 256).astype(BF))
    codes_top = codes_top.at[1, :rows].set((top_target % 256).astype(BF))
    own_quarter = lax.dynamic_slice_in_dim(top_weight, dp_at * quarter, quarter, 0)
    sent = jnp.concatenate([queries, own_quarter, codes_top], axis=0)
    sent, got = lax.optimization_barrier((sent, got))

    def along(step):
        return [
            (z * 2 + x, ((z - step) % steps) * 2 + x) for z in range(steps) for x in range(2)
        ]

    mine = jnp.stack([sent] + [lax.ppermute(sent, "label", along(n)) for n in range(1, steps)])
    other = lax.ppermute(mine, "label", [(i, i ^ 1) for i in range(label_size)])
    w_near = jnp.concatenate([mine[:, rows : rows + quarter], other[:, rows : rows + quarter]])
    w_near = w_near.reshape(label_size * quarter, width)
    w_y = lax.ppermute(w_near, "dp", [(i, i ^ 2) for i in range(dp_size)])
    w_core = lax.ppermute(
        jnp.concatenate([w_near, w_y]), "dp", [(i, i ^ 1) for i in range(dp_size)]
    )
    z_at, x_at = label_at // 2, label_at % 2
    source = jnp.concatenate(
        [((z_at + jnp.arange(steps)) % steps) * 2 + x_at, ((z_at + jnp.arange(steps)) % steps) * 2 + 1 - x_at]
    )
    dp_source = jnp.stack([dp_at, dp_at ^ 2, dp_at ^ 1, dp_at ^ 3])
    own_column = (
        source[None, :, None] * held_top
        + dp_source[:, None, None] * quarter
        + jnp.arange(quarter)[None, None, :]
    ).reshape(1, dp_size * label_size * quarter)
    top_back, top_part, top_loss = call(
        functools.partial(top_kernel, rows=rows, quarter=quarter),
        (shape((rows, width), F32), shape((held_top, width), F32), shape((SUB, rows), F32)),
        (
            (label_at * held_top).astype(jnp.int32)[None],
            mine,
            other,
            w_y,
            w_core,
            own_column.astype(F32),
            top_weight,
        ),
        scratch=(pltpu.VMEM((label_size * held_top, width), BF),),
        scalars=1,
        name="top",
    )
    core = dp_at % 2
    half = held_top // 2
    both = top_part + lax.ppermute(top_part, "dp", [(i, i ^ 1) for i in range(dp_size)])
    share = lax.dynamic_slice_in_dim(both, core * half, half, 0)
    share = share + lax.ppermute(share, "dp", [(i, i ^ 2) for i in range(dp_size)])
    rest = lax.ppermute(share, "dp", [(i, i ^ 1) for i in range(dp_size)])
    low = jnp.where(core == 0, share, rest)
    high = jnp.where(core == 0, rest, share)
    top_grad = jnp.concatenate([low, high])

    query_grad = call(
        functools.partial(finish_kernel, held=held, short_len=short_len),
        shape((rows, width), F32),
        (info, returned, top_back),
        name="finish",
    )
    losses = jnp.concatenate([top_loss[:1], pair_losses[:2]])
    return (query_grad, top_grad, mid_grad, leaf_grad, losses)


def solution(mesh):
    in_specs = (
        P(("dp", "label"), None),
        P(("dp", "label"), None),
        P(),
        P(("dp", "label")),
        P(("dp", "label")),
        P("label", None),
        P(("dp", "label"), None),
        P(("dp", "label"), None, None),
    )
    out_specs = (
        P(("dp", "label"), None),
        P("label", None),
        P(("dp", "label"), None),
        P(("dp", "label"), None, None),
        P(None, ("dp", "label")),
    )
    return jax.shard_map(
        per_device, mesh=mesh, in_specs=in_specs, out_specs=out_specs, check_vma=False
    )
```

```python
import functools

import jax
import jax.numpy as jnp
from jax import lax
from jax.experimental import pallas as pl
from jax.experimental.pallas import tpu as pltpu
from jax.sharding import PartitionSpec as P

D = 512
BLOCKS = 512
CAPB = 2


def shortened(array):

    def short(part):
        return part.astype(jnp.bfloat16) if part.dtype == jnp.float32 else part

    return jax.tree.map(short, array)


def route_narrow(payload):
    return jax.tree.map(
        lambda part, own: part.astype(own.dtype),
        lax.all_to_all(
            lax.all_to_all(shortened(payload), "label", split_axis=1, concat_axis=1, tiled=True),
            "dp",
            split_axis=0,
            concat_axis=0,
            tiled=True,
        ),
        payload,
    )


def route_wide(payload):
    return lax.all_to_all(
        lax.all_to_all(payload, "label", split_axis=1, concat_axis=1, tiled=True),
        "dp",
        split_axis=0,
        concat_axis=0,
        tiled=True,
    )


def per_device_any(
    queries, shortlist, slab_slot, top_target, leaf_target, top_weight, mid_weight, leaf_weight
):
    dp_size = lax.axis_size("dp")
    label_size = lax.axis_size("label")
    rows_here = queries.shape[0]
    short_len = shortlist.shape[1]
    block_dev = leaf_weight.shape[0]
    all_rows = lax.all_gather(top_weight, "label", axis=0, tiled=True)
    scores = jnp.dot(queries, all_rows.T, preferred_element_type=jnp.float32)
    totals = jax.nn.logsumexp(scores, axis=1)
    target_hit = top_target[:, None] == jnp.arange(scores.shape[1], dtype=jnp.int32)[None, :]
    top_loss = totals - jnp.sum(jnp.where(target_hit, scores, 0.0), axis=1)
    dscore = (jnp.exp(scores - totals[:, None]) - target_hit.astype(jnp.float32)).astype(
        jnp.bfloat16
    )
    top_back = jnp.dot(dscore, all_rows, preferred_element_type=jnp.float32)
    columns_held = lax.all_to_all(dscore, "label", split_axis=1, concat_axis=0, tiled=True)
    top_part = lax.dot_general(
        columns_held,
        lax.all_gather(queries, "label", axis=0, tiled=True),
        (((0,), (0,)), ((), ())),
        preferred_element_type=jnp.float32,
    )
    top_grad = lax.psum(top_part, "dp")
    position = slab_slot[shortlist].reshape(-1)
    sort_order = jnp.argsort(position, stable=True)
    ranked = position[sort_order]
    run_start = jnp.searchsorted(ranked, ranked, side="left")
    slot_rank = jnp.arange(ranked.shape[0], dtype=jnp.int32) - run_start
    slot_of = jnp.zeros_like(position).at[sort_order].set(ranked * CAPB + slot_rank)
    first_slot = (jnp.arange(short_len, dtype=jnp.int32) == 0)[None, :]
    pair_codes = jnp.where(first_slot, leaf_target[:, None], -1).reshape(-1).astype(jnp.float32)
    layout = (dp_size, label_size, block_dev, CAPB)
    send_rows = (
        jnp.zeros((BLOCKS * CAPB, D), jnp.bfloat16)
        .at[slot_of]
        .set(jnp.repeat(queries, short_len, axis=0))
    )
    send_code = (
        jnp.full((BLOCKS * CAPB,), -2.0, jnp.float32)
        .at[slot_of]
        .set(pair_codes)
        .astype(jnp.bfloat16)
    )
    got_rows, got_code = route_narrow((send_rows.reshape(layout + (D,)), send_code.reshape(layout)))
    scores_held = jnp.einsum(
        "abkcd,kld->abkcl", got_rows, leaf_weight, preferred_element_type=jnp.float32
    )
    mid_held = jnp.einsum(
        "abkcd,kd->abkc", got_rows, mid_weight, preferred_element_type=jnp.float32
    )
    block_lse = jax.nn.logsumexp(scores_held, axis=-1)
    code_float = got_code.astype(jnp.float32)
    labels = jnp.arange(scores_held.shape[-1], dtype=jnp.float32)
    target_hit = (code_float[..., None] == labels).astype(jnp.float32)
    target_held = jnp.sum(scores_held * target_hit, axis=-1)
    back_mid, back_lse, back_target = route_wide((mid_held, block_lse, target_held))
    pair_mid = back_mid.reshape(-1)[slot_of].reshape(rows_here, short_len)
    pair_lse = back_lse.reshape(-1)[slot_of].reshape(rows_here, short_len)
    pair_target = back_target.reshape(-1)[slot_of].reshape(rows_here, short_len)
    mid_totals = jax.nn.logsumexp(pair_mid, axis=1)
    mid_loss = mid_totals - pair_mid[:, 0]
    mid_delta = (jnp.exp(pair_mid - mid_totals[:, None]) - first_slot.astype(jnp.float32)).astype(
        jnp.bfloat16
    )
    leaf_lse = jax.nn.logsumexp(pair_lse, axis=1)
    leaf_loss = leaf_lse - pair_target[:, 0]
    send_delta = (
        jnp.zeros((BLOCKS * CAPB,), jnp.float32)
        .at[slot_of]
        .set(mid_delta.reshape(-1).astype(jnp.float32))
    )
    send_lse = (
        jnp.zeros((BLOCKS * CAPB,), jnp.float32).at[slot_of].set(jnp.repeat(leaf_lse, short_len))
    )
    got_delta, got_lse = route_wide((send_delta.reshape(layout), send_lse.reshape(layout)))
    live_slot = code_float > -1.5
    leaf_delta = jnp.where(
        live_slot[..., None], jnp.exp(scores_held - got_lse[..., None]) - target_hit, 0.0
    ).astype(jnp.bfloat16)
    mid_slots = got_delta.astype(jnp.bfloat16)
    leaf_grad = jnp.einsum(
        "abkcl,abkcd->kld", leaf_delta, got_rows, preferred_element_type=jnp.float32
    )
    mid_grad = jnp.einsum("abkc,abkcd->kd", mid_slots, got_rows, preferred_element_type=jnp.float32)
    pair_back = jnp.einsum(
        "abkcl,kld->abkcd", leaf_delta, leaf_weight, preferred_element_type=jnp.float32
    )
    pair_back = (
        pair_back
        + mid_slots.astype(jnp.float32)[..., None] * mid_weight.astype(jnp.float32)[:, None, :]
    ).astype(jnp.bfloat16)
    returned = route_narrow(pair_back)
    pair_sum = (
        returned.reshape(BLOCKS * CAPB, D)[slot_of]
        .astype(jnp.float32)
        .reshape(rows_here, short_len, D)
        .sum(axis=1)
    )
    query_grad = top_back + pair_sum
    losses = jnp.stack([top_loss, mid_loss, leaf_loss])
    return (query_grad, top_grad, mid_grad, leaf_grad, losses)


LANES = 128
SUB = 8
BF = jnp.bfloat16
F32 = jnp.float32
HIGH = lax.Precision.HIGHEST


def params(mib):
    return pltpu.CompilerParams(vmem_limit_bytes=mib * 1024 * 1024)


def iota(shape, dim):
    return lax.broadcasted_iota(jnp.int32, shape, dim)


def iota_f(shape, dim):
    return iota(shape, dim).astype(F32)


def dot_nn(a, b, precision=None):
    return lax.dot_general(
        a, b, (((1,), (0,)), ((), ())), precision=precision, preferred_element_type=F32
    )


def dot_nt(a, b, precision=None):
    return lax.dot_general(
        a, b, (((1,), (1,)), ((), ())), precision=precision, preferred_element_type=F32
    )


def dot_tn(a, b, precision=None):
    return lax.dot_general(
        a, b, (((0,), (0,)), ((), ())), precision=precision, preferred_element_type=F32
    )


def pack_kernel(
    q_ref, short_ref, slab_ref, leaf_t_ref, top_t_ref, pay_ref, info_ref, own_ref, *, devs, held
):
    rows, width = q_ref.shape
    short_len = short_ref.shape[0]
    clusters = slab_ref.shape[1]
    chunks = width // LANES
    slots = CAPB * held
    cluster_f = iota_f((rows, clusters), 1)
    slab = jnp.broadcast_to(slab_ref[...].astype(F32), (rows, clusters))
    short = short_ref[...].astype(F32)
    short = jnp.concatenate([short, jnp.zeros((rows - short_len, rows), F32)], axis=0).T
    places, hits = [], []
    for j in range(short_len):
        place = jnp.sum(jnp.where(short[:, j : j + 1] == cluster_f, slab, 0.0), axis=1, keepdims=True)
        places.append(place)
        hits.append(jnp.where(place == cluster_f, 1.0, 0.0))
    hit = functools.reduce(lambda a, b: a + b, hits)
    before = jnp.where(iota((rows, rows), 1) < iota((rows, rows), 0), 1.0, 0.0).astype(BF)
    count = dot_nn(before, hit.astype(BF))
    lane = iota((rows, LANES), 1)
    info = jnp.zeros((rows, LANES), F32)
    for j in range(short_len):
        rank = jnp.sum(hits[j] * count, axis=1, keepdims=True)
        info = jnp.where(lane == j, places[j], info)
        info = jnp.where(lane == short_len + j, rank, info)
    info_ref[...] = info
    queries = q_ref[...]
    own_ref[:rows, :] = queries
    top_target = jnp.broadcast_to(top_t_ref[...].astype(F32), (16, rows))
    high = jnp.floor(top_target * (1.0 / 256.0))
    code_at = iota((16, rows), 0)
    coded = jnp.where(code_at == 0, high, jnp.where(code_at == 1, top_target - 256.0 * high, 0.0))
    own_ref[rows:, :] = jnp.concatenate([coded] * chunks, axis=1).astype(BF)
    target = jnp.broadcast_to(leaf_t_ref[...].astype(F32) + 1.0, (SUB, rows)).astype(BF)
    ones = jnp.ones((SUB, rows), BF)
    table_rows = clusters // LANES
    table = jnp.zeros((CAPB * table_rows, LANES), F32)
    sub = iota((CAPB * table_rows, LANES), 0)
    for r in range(CAPB):
        pick = jnp.where(count == float(r), hit, 0.0)
        chosen = pick.astype(BF)
        first = (pick * hits[0]).astype(BF)
        code = dot_nn(ones, chosen) + dot_nn(target, first)
        for i in range(table_rows):
            part = jnp.broadcast_to(code[0:1, i * LANES : (i + 1) * LANES], table.shape)
            table = jnp.where(sub == r * table_rows + i, part, table)
        got = dot_tn(chosen, queries).astype(BF)
        for c in range(chunks):
            start = c * slots + r * held
            pay_ref[:, start : start + held, :] = got[:, c * LANES : (c + 1) * LANES].reshape(
                devs, held, LANES
            )
    coded = table.astype(BF)
    pay_ref[:, chunks * slots :, :] = jnp.broadcast_to(coded[None], (devs,) + coded.shape)


def halves(source, target, sems):
    half = source.shape[0] // 2
    return [
        pltpu.make_async_copy(
            source.at[pl.ds(n * half, half)], target.at[pl.ds(n * half, half)], sems.at[n]
        )
        for n in range(2)
    ]


def start(copies):
    for copy in copies:
        copy.start()
    return copies


def forward_kernel(
    me_ref, got_ref, leaf_in, mid_ref, rows_out, score_out, stat_ref,
    wide_ref, table_ref, leaf_ref, rows_ref, score_ref, leaf_sem, rows_sem, score_sem,
):
    devs, depth, _ = got_ref.shape
    held, labels, width = leaf_ref.shape
    fetches = start(halves(leaf_in, leaf_ref, leaf_sem))
    sends = list(zip(halves(rows_ref, rows_out, rows_sem), halves(score_ref, score_out, score_sem)))
    chunks = width // LANES
    slots = CAPB * held
    body = chunks * slots
    wide_ref[...] = got_ref[:, :body, :].reshape(devs * body, LANES).astype(F32)
    tail = depth - body
    table_ref[...] = got_ref[:, body:, :].astype(F32).reshape(devs * tail, LANES)
    first = me_ref[0] * held
    row_at = first // LANES
    lane_at = first - row_at * LANES
    lane = iota((devs, LANES), 1)
    codes = jnp.zeros((devs, LANES), F32)
    for r in range(CAPB):
        row = table_ref[pl.ds(r * (tail // CAPB) + row_at, devs, stride=tail), :]
        row = pltpu.roll(row, lax.rem(r * held - lane_at + LANES, LANES), 1)
        codes = jnp.where((lane >= r * held) & (lane < (r + 1) * held), row, codes)
    stat_ref[pl.ds(1, devs, stride=SUB), :] = codes
    label_f = iota_f((CAPB * devs, labels), 1)
    stats = jnp.zeros((devs, LANES), F32)
    for k in range(held):
        parts = []
        for r in range(CAPB):
            parts.append(
                jnp.concatenate(
                    [
                        wide_ref[pl.ds(c * slots + r * held + k, devs, stride=body), :]
                        for c in range(chunks)
                    ],
                    axis=1,
                )
            )
        full = jnp.concatenate(parts, axis=0)
        rows = full.astype(BF)
        rows_ref[k] = rows
        if k % (held // 2) == 0:
            fetches[k // (held // 2)].wait()
        scores = dot_nt(rows, leaf_ref[k])
        score_ref[k] = scores
        mid = jnp.sum(full * mid_ref[k : k + 1, :].astype(F32), axis=1, keepdims=True)
        peak = jnp.max(scores, axis=1, keepdims=True)
        lse = peak + jnp.log(jnp.sum(jnp.exp(scores - peak), axis=1, keepdims=True))
        code = jnp.concatenate(
            [codes[:, r * held + k : r * held + k + 1] for r in range(CAPB)], axis=0
        )
        target = jnp.sum(jnp.where(code - 2.0 == label_f, scores, 0.0), axis=1, keepdims=True)
        for n, value in enumerate((mid, lse, target)):
            for r in range(CAPB):
                stats = jnp.where(
                    lane == n * slots + r * held + k, value[r * devs : (r + 1) * devs], stats
                )
        if (k + 1) % (held // 2) == 0:
            start(sends[k // (held // 2)])
    stat_ref[pl.ds(0, devs, stride=SUB), :] = stats
    for pair in sends:
        for send in pair:
            send.wait()


def middle_kernel(info_ref, stat_ref, out_ref, loss_ref, *, devs, held, short_len):
    rows = info_ref.shape[0]
    slots = CAPB * held
    info = info_ref[...]
    stats = stat_ref[pl.ds(0, devs, stride=SUB), :]
    lane = iota_f((rows, LANES), 1)
    dev_f = iota_f((rows, devs), 1)
    owners, spots, mids, lses = [], [], [], []
    for j in range(short_len):
        place = info[:, j : j + 1]
        rank = info[:, short_len + j : short_len + j + 1]
        dev = jnp.floor(place * (1.0 / held))
        spot = place - dev * held + rank * held
        owner = jnp.where(dev == dev_f, 1.0, 0.0)
        values = dot_nn(owner, stats, HIGH)
        owners.append(owner)
        spots.append(spot)
        mids.append(jnp.sum(jnp.where(lane == spot, values, 0.0), axis=1, keepdims=True))
        lses.append(jnp.sum(jnp.where(lane == spot + slots, values, 0.0), axis=1, keepdims=True))
        if j == 0:
            target = jnp.sum(
                jnp.where(lane == spot + 2 * slots, values, 0.0), axis=1, keepdims=True
            )

    def total(columns):
        peak = functools.reduce(jnp.maximum, columns)
        return peak + jnp.log(functools.reduce(lambda a, b: a + b, [jnp.exp(v - peak) for v in columns]))

    mid_total = total(mids)
    leaf_total = total(lses)
    back = []
    for j in range(short_len):
        delta = jnp.exp(mids[j] - mid_total) - (1.0 if j == 0 else 0.0)
        delta = delta.astype(BF).astype(F32)
        back.append(
            jnp.where(
                lane == spots[j], leaf_total, jnp.where(lane == spots[j] + slots, delta, 0.0)
            )
        )
    sent = dot_tn(jnp.concatenate(owners, axis=0), jnp.concatenate(back, axis=0), HIGH)
    out_ref[pl.ds(0, devs, stride=SUB), :] = sent
    losses = jnp.where(lane == 0.0, mid_total - mids[0], jnp.where(lane == 1.0, leaf_total - target, 0.0))
    loss_ref[...] = losses.T[:SUB, :]


def backward_kernel(
    score_in, stat_ref, norm_ref, leaf_in, mid_ref, delta_ref, pay_out,
    wide_ref, score_ref, leaf_ref, pay_ref, score_sem, leaf_sem, pay_sem,
):
    held, pairs, labels = score_ref.shape
    fetches = start(halves(score_in, score_ref, score_sem))
    leaf_fetches = start(halves(leaf_in, leaf_ref, leaf_sem))
    devs = pairs // CAPB
    width = leaf_ref.shape[2]
    chunks = width // LANES
    slots = CAPB * held
    body = chunks * slots
    norms = norm_ref[pl.ds(0, devs, stride=SUB), :]
    codes = stat_ref[pl.ds(1, devs, stride=SUB), :]
    label_f = iota_f((pairs, labels), 1)

    def column(array, base, k):
        return jnp.concatenate(
            [array[:, base + r * held + k : base + r * held + k + 1] for r in range(CAPB)], axis=0
        )

    for k in range(held):
        code = column(codes, 0, k)
        lse = column(norms, 0, k)
        mid_delta = column(norms, slots, k)
        onehot = jnp.where(code - 2.0 == label_f, 1.0, 0.0)
        if k % (held // 2) == 0:
            fetches[k // (held // 2)].wait()
            leaf_fetches[k // (held // 2)].wait()
        delta = jnp.where(code > 0.5, jnp.exp(score_ref[k] - lse) - onehot, 0.0).astype(BF)
        delta_ref[k] = delta
        back = dot_nn(delta, leaf_ref[k]) + mid_delta * mid_ref[k : k + 1, :].astype(F32)
        for r in range(CAPB):
            for c in range(chunks):
                wide_ref[pl.ds(c * slots + r * held + k, devs, stride=body), :] = back[
                    r * devs : (r + 1) * devs, c * LANES : (c + 1) * LANES
                ]
    sends = []
    for g in range(0, devs, SUB):
        pay_ref[g : g + SUB] = (
            wide_ref[g * body : (g + SUB) * body, :].astype(BF).reshape(SUB, body, LANES)
        )
        sends.append(
            pltpu.make_async_copy(
                pay_ref.at[pl.ds(g, SUB)], pay_out.at[pl.ds(g, SUB)], pay_sem.at[g // SUB]
            )
        )
        sends[-1].start()
    for send in sends:
        send.wait()


def grads_kernel(delta_ref, norm_ref, rows_ref, leaf_grad_ref, mid_grad_ref):
    held, pairs, _ = delta_ref.shape
    devs = pairs // CAPB
    slots = CAPB * held
    norms = norm_ref[pl.ds(0, devs, stride=SUB), :]
    for k in range(held):
        rows = rows_ref[k]
        leaf_grad_ref[k] = dot_tn(delta_ref[k], rows)
        mid_delta = jnp.concatenate(
            [norms[:, slots + r * held + k : slots + r * held + k + 1] for r in range(CAPB)], axis=0
        )
        mid_grad_ref[k : k + 1, :] = jnp.sum(mid_delta * rows.astype(F32), axis=0, keepdims=True)


def finish_kernel(info_ref, back_ref, top_ref, out_ref, *, held, short_len):
    rows, width = out_ref.shape
    devs = back_ref.shape[0]
    clusters = devs * held
    chunks = width // LANES
    slots = CAPB * held
    info = info_ref[...]
    cluster_f = iota_f((rows, clusters), 1)
    picks = []
    for r in range(CAPB):
        pick = jnp.zeros((rows, clusters), F32)
        for j in range(short_len):
            place = jnp.where(
                info[:, short_len + j : short_len + j + 1] == float(r), info[:, j : j + 1], -1.0
            )
            pick = jnp.where(place == cluster_f, 1.0, pick)
        picks.append(pick.astype(BF))
    for c in range(chunks):
        total = top_ref[:, c * LANES : (c + 1) * LANES]
        for r in range(CAPB):
            start = c * slots + r * held
            total = total + dot_nn(
                picks[r], back_ref[:, start : start + held, :].reshape(clusters, LANES)
            )
        out_ref[:, c * LANES : (c + 1) * LANES] = total


def top_step(block, target, weights, weight_held, held_base):
    scores = dot_nt(block, weights)
    peak = jnp.max(scores, axis=1, keepdims=True)
    total = peak + jnp.log(jnp.sum(jnp.exp(scores - peak), axis=1, keepdims=True))
    mine = dot_nt(block, weight_held)
    held_f = iota_f(mine.shape, 1) + held_base
    delta = (jnp.exp(mine - total) - jnp.where(target == held_f, 1.0, 0.0)).astype(BF)
    return scores, total, dot_tn(delta, block)


def top_column(codes):
    target = codes[0:1, :LANES].astype(F32) * 256.0 + codes[1:2, :LANES].astype(F32)
    return jnp.broadcast_to(target, (LANES, LANES)).T[:, 0:1]


def top_own_kernel(
    where_ref, own_ref, near_ref, other_ref, wy_ref, wc_ref, column_ref, weight_ref,
    back_ref, part_ref, loss_ref, all_ref,
):
    rows = own_ref.shape[0] - 16
    piece = near_ref.shape[0]
    all_ref[:piece, :] = near_ref[...]
    all_ref[piece : 2 * piece, :] = other_ref[...]
    all_ref[2 * piece : 4 * piece, :] = wy_ref[...]
    all_ref[4 * piece :, :] = wc_ref[...]
    block = own_ref[:rows, :]
    target = top_column(own_ref[rows:, :])
    scores, total, part = top_step(
        block, target, all_ref[...], weight_ref[...], where_ref[0].astype(F32)
    )
    part_ref[...] = part
    hit = jnp.broadcast_to(column_ref[...], scores.shape) == target
    full = (jnp.exp(scores - total) - jnp.where(hit, 1.0, 0.0)).astype(BF)
    back_ref[...] = dot_nn(full, all_ref[...])
    loss = total - jnp.sum(jnp.where(hit, scores, 0.0), axis=1, keepdims=True)
    loss_ref[...] = jnp.broadcast_to(loss, (rows, LANES)).T[:SUB, :]


def top_more_kernel(where_ref, blocks_ref, all_ref, weight_ref, part_ref, out_ref, *, first):
    count, depth, _ = blocks_ref.shape
    rows = depth - 16
    numbers = range(first, count)
    block = jnp.concatenate([blocks_ref[n, :rows, :] for n in numbers], axis=0)
    target = jnp.concatenate([top_column(blocks_ref[n, rows:, :]) for n in numbers], axis=0)
    base = where_ref[0].astype(F32)
    part = top_step(block, target, all_ref[...], weight_ref[...], base)[2]
    out_ref[...] = part_ref[...] + part


def spec():
    return pl.BlockSpec(memory_space=pltpu.VMEM)


def call(kernel, outs, ins, scratch=(), scalars=0, far_ins=(), far_outs=(), mib=58, name=None):
    far = pl.BlockSpec(memory_space=pltpu.HBM)
    small = pl.BlockSpec(memory_space=pltpu.SMEM)
    listed = isinstance(outs, tuple)
    out_specs = tuple(
        far if n in far_outs else spec() for n in range(len(outs) if listed else 1)
    )
    return pl.pallas_call(
        kernel,
        out_shape=outs,
        in_specs=[
            small if n < scalars else far if n in far_ins else spec() for n in range(len(ins))
        ],
        out_specs=out_specs if listed else out_specs[0],
        scratch_shapes=list(scratch),
        compiler_params=params(mib),
        name=name,
    )(*ins)


def shape(dims, dtype):
    return jax.ShapeDtypeStruct(dims, dtype)


def fits(queries, leaf_weight, shortlist, top_weight, devs, dp_size, label_size):
    rows, width = queries.shape
    held, labels = leaf_weight.shape[:2]
    return (
        rows == LANES
        and labels == LANES
        and width % LANES == 0
        and held % 16 == 0
        and LANES % held == 0
        and 3 * CAPB * held <= LANES
        and CAPB * (devs * held // LANES) % SUB == 0
        and devs % SUB == 0
        and dp_size == 4
        and label_size == 8
        and top_weight.shape[0] % (dp_size * 16) == 0
        and top_weight.shape[0] * label_size <= 65536
        and 2 * shortlist.shape[1] <= LANES
    )


def after(value, first):
    return lax.optimization_barrier((value, first))[0]


def exchange(array):
    return lax.all_to_all(array, ("dp", "label"), split_axis=0, concat_axis=0, tiled=True)


def per_device(
    queries, shortlist, slab_slot, top_target, leaf_target, top_weight, mid_weight, leaf_weight
):
    dp_size = lax.axis_size("dp")
    label_size = lax.axis_size("label")
    devs = dp_size * label_size
    if not fits(queries, leaf_weight, shortlist, top_weight, devs, dp_size, label_size):
        return per_device_any(
            queries, shortlist, slab_slot, top_target, leaf_target, top_weight, mid_weight, leaf_weight
        )
    rows, width = queries.shape
    held, labels = leaf_weight.shape[:2]
    short_len = shortlist.shape[1]
    clusters = devs * held
    chunks = width // LANES
    slots = CAPB * held
    body = chunks * slots
    tail = CAPB * clusters // LANES
    dp_at = lax.axis_index("dp")
    label_at = lax.axis_index("label")
    me = dp_at * label_size + label_at

    steps = label_size // 2
    quarter = top_weight.shape[0] // dp_size
    held_top = top_weight.shape[0]
    flip_x = [(i, i ^ 1) for i in range(label_size)]
    flip_y = [(i, i ^ 2) for i in range(dp_size)]
    flip_core = [(i, i ^ 1) for i in range(dp_size)]

    def along(step):
        return [
            (z * 2 + x, ((z - step) % steps) * 2 + x) for z in range(steps) for x in range(2)
        ]

    own_quarter = lax.dynamic_slice_in_dim(top_weight, dp_at * quarter, quarter, 0)
    w_near = jnp.concatenate(
        [own_quarter] + [lax.ppermute(own_quarter, "label", along(n)) for n in range(1, steps)]
    )
    me = me.astype(jnp.int32)[None]
    label_base = (label_at * held_top).astype(jnp.int32)[None]
    payload, info, own = call(
        functools.partial(pack_kernel, devs=devs, held=held),
        (
            shape((devs, body + tail, LANES), BF),
            shape((rows, LANES), F32),
            shape((rows + 16, width), BF),
        ),
        (
            after(queries, (me, label_base)),
            shortlist.T,
            slab_slot[None, :],
            leaf_target[None, :],
            top_target[None, :],
        ),
        name="pack",
    )
    payload = after(payload, w_near)
    got = exchange(payload)
    w_other = lax.ppermute(w_near, "label", flip_x)
    w_y = lax.ppermute(jnp.concatenate([w_near, w_other]), "dp", flip_y)
    z_at, x_at = label_at // 2, label_at % 2
    source = (z_at + jnp.arange(steps)) % steps * 2
    source = jnp.concatenate([source + x_at, source + 1 - x_at])
    dp_source = jnp.stack([dp_at, dp_at ^ 2, dp_at ^ 1, dp_at ^ 3])
    own_column = (
        source[None, :, None] * held_top
        + dp_source[:, None, None] * quarter
        + jnp.arange(quarter)[None, None, :]
    ).reshape(1, dp_size * label_size * quarter)
    sent = after(own, got)
    peers = [lax.ppermute(sent, "label", along(n)) for n in range(1, steps)]
    pairs = CAPB * devs
    rows_held, scores, stats = call(
        forward_kernel,
        (
            shape((held, pairs, width), BF),
            shape((held, pairs, labels), F32),
            shape((devs * SUB, LANES), F32),
        ),
        (me, got, leaf_weight, mid_weight),
        scratch=(
            pltpu.VMEM((devs * body, LANES), F32),
            pltpu.VMEM((devs * tail, LANES), F32),
            pltpu.VMEM((held, labels, width), BF),
            pltpu.VMEM((held, pairs, width), BF),
            pltpu.VMEM((held, pairs, labels), F32),
            pltpu.SemaphoreType.DMA((2,)),
            pltpu.SemaphoreType.DMA((2,)),
            pltpu.SemaphoreType.DMA((2,)),
        ),
        scalars=1,
        far_ins=(2,),
        far_outs=(0, 1),
        name="forward",
    )
    w_y = after(w_y, stats)
    w_core = lax.ppermute(jnp.concatenate([w_near, w_other, w_y]), "dp", flip_core)
    stats_back = exchange(stats.reshape(devs, SUB, LANES)).reshape(devs * SUB, LANES)
    norms, pair_losses = call(
        functools.partial(middle_kernel, devs=devs, held=held, short_len=short_len),
        (shape((devs * SUB, LANES), F32), shape((SUB, rows), F32)),
        (info, stats_back),
        mib=16,
        name="middle",
    )
    norms_held = exchange(norms.reshape(devs, SUB, LANES)).reshape(devs * SUB, LANES)
    top_back, top_part, top_loss, top_all = call(
        top_own_kernel,
        (
            shape((rows, width), F32),
            shape((held_top, width), F32),
            shape((SUB, rows), F32),
            shape((label_size * held_top, width), BF),
        ),
        (label_base, own, after(w_near, norms), w_other, w_y, w_core, own_column.astype(F32), top_weight),
        scalars=1,
        name="top_own",
    )
    mine = jnp.stack([sent] + after(peers, top_part))
    other = lax.ppermute(mine, "label", flip_x)
    norms_held = after(norms_held, top_part)
    delta, back = call(
        backward_kernel,
        (shape((held, pairs, labels), BF), shape((devs, body, LANES), BF)),
        (scores, stats, norms_held, leaf_weight, mid_weight),
        scratch=(
            pltpu.VMEM((devs * body, LANES), F32),
            pltpu.VMEM((held, pairs, labels), F32),
            pltpu.VMEM((held, labels, width), BF),
            pltpu.VMEM((devs, body, LANES), BF),
            pltpu.SemaphoreType.DMA((2,)),
            pltpu.SemaphoreType.DMA((2,)),
            pltpu.SemaphoreType.DMA((devs // SUB,)),
        ),
        far_ins=(0, 3),
        far_outs=(1,),
        name="backward",
    )
    returned = exchange(back)
    top_part = call(
        functools.partial(top_more_kernel, first=1),
        shape((held_top, width), F32),
        (label_base, after(mine, back), top_all, top_weight, top_part),
        scalars=1,
        name="top_near",
    )
    top_part = call(
        functools.partial(top_more_kernel, first=0),
        shape((held_top, width), F32),
        (label_base, after(other, back), top_all, top_weight, top_part),
        scalars=1,
        name="top_far",
    )
    losses = jnp.concatenate([top_loss[:1], pair_losses[:2]])
    core = dp_at % 2
    half = held_top // 2
    both = top_part + lax.ppermute(top_part, "dp", flip_core)
    share = lax.dynamic_slice_in_dim(both, core * half, half, 0)
    from_y = lax.ppermute(share, "dp", flip_y)
    leaf_grad, mid_grad = call(
        grads_kernel,
        (shape((held, labels, width), F32), shape((held, width), F32)),
        (delta, norms_held, after(rows_held, (share, losses))),
        name="grads",
    )
    share = share + after(from_y, mid_grad)
    rest = lax.ppermute(share, "dp", flip_core)
    top_grad = jnp.concatenate(
        [jnp.where(core == 0, share, rest), jnp.where(core == 0, rest, share)]
    )
    query_grad = call(
        functools.partial(finish_kernel, held=held, short_len=short_len),
        shape((rows, width), F32),
        (info, returned, top_back),
        mib=16,
        name="finish",
    )
    return (query_grad, top_grad, mid_grad, leaf_grad, losses)


def solution(mesh):
    in_specs = (
        P(("dp", "label"), None),
        P(("dp", "label"), None),
        P(),
        P(("dp", "label")),
        P(("dp", "label")),
        P("label", None),
        P(("dp", "label"), None),
        P(("dp", "label"), None, None),
    )
    out_specs = (
        P(("dp", "label"), None),
        P("label", None),
        P(("dp", "label"), None),
        P(("dp", "label"), None, None),
        P(None, ("dp", "label")),
    )
    return jax.shard_map(
        per_device, mesh=mesh, in_specs=in_specs, out_specs=out_specs, check_vma=False
    )
```

```python
import functools

import jax
import jax.numpy as jnp
from jax import lax
from jax.experimental import pallas as pl
from jax.experimental.pallas import tpu as pltpu
from jax.sharding import PartitionSpec as P


D = 512
BLOCKS = 512
CAPB = 2


def shortened(array):

    def short(part):
        return part.astype(jnp.bfloat16) if part.dtype == jnp.float32 else part

    return jax.tree.map(short, array)


def route_narrow(payload):
    return jax.tree.map(
        lambda part, own: part.astype(own.dtype),
        lax.all_to_all(
            lax.all_to_all(shortened(payload), "label", split_axis=1, concat_axis=1, tiled=True),
            "dp",
            split_axis=0,
            concat_axis=0,
            tiled=True,
        ),
        payload,
    )


def route_wide(payload):
    return lax.all_to_all(
        lax.all_to_all(payload, "label", split_axis=1, concat_axis=1, tiled=True),
        "dp",
        split_axis=0,
        concat_axis=0,
        tiled=True,
    )


def per_device_any(
    queries, shortlist, slab_slot, top_target, leaf_target, top_weight, mid_weight, leaf_weight
):
    dp_size = lax.axis_size("dp")
    label_size = lax.axis_size("label")
    rows_here = queries.shape[0]
    short_len = shortlist.shape[1]
    block_dev = leaf_weight.shape[0]
    all_rows = lax.all_gather(top_weight, "label", axis=0, tiled=True)
    scores = jnp.dot(queries, all_rows.T, preferred_element_type=jnp.float32)
    totals = jax.nn.logsumexp(scores, axis=1)
    target_hit = top_target[:, None] == jnp.arange(scores.shape[1], dtype=jnp.int32)[None, :]
    top_loss = totals - jnp.sum(jnp.where(target_hit, scores, 0.0), axis=1)
    dscore = (jnp.exp(scores - totals[:, None]) - target_hit.astype(jnp.float32)).astype(
        jnp.bfloat16
    )
    top_back = jnp.dot(dscore, all_rows, preferred_element_type=jnp.float32)
    columns_held = lax.all_to_all(dscore, "label", split_axis=1, concat_axis=0, tiled=True)
    top_part = lax.dot_general(
        columns_held,
        lax.all_gather(queries, "label", axis=0, tiled=True),
        (((0,), (0,)), ((), ())),
        preferred_element_type=jnp.float32,
    )
    top_grad = lax.psum(top_part, "dp")
    position = slab_slot[shortlist].reshape(-1)
    sort_order = jnp.argsort(position, stable=True)
    ranked = position[sort_order]
    run_start = jnp.searchsorted(ranked, ranked, side="left")
    slot_rank = jnp.arange(ranked.shape[0], dtype=jnp.int32) - run_start
    slot_of = jnp.zeros_like(position).at[sort_order].set(ranked * CAPB + slot_rank)
    first_slot = (jnp.arange(short_len, dtype=jnp.int32) == 0)[None, :]
    pair_codes = jnp.where(first_slot, leaf_target[:, None], -1).reshape(-1).astype(jnp.float32)
    layout = (dp_size, label_size, block_dev, CAPB)
    send_rows = (
        jnp.zeros((BLOCKS * CAPB, D), jnp.bfloat16)
        .at[slot_of]
        .set(jnp.repeat(queries, short_len, axis=0))
    )
    send_code = (
        jnp.full((BLOCKS * CAPB,), -2.0, jnp.float32)
        .at[slot_of]
        .set(pair_codes)
        .astype(jnp.bfloat16)
    )
    got_rows, got_code = route_narrow((send_rows.reshape(layout + (D,)), send_code.reshape(layout)))
    scores_held = jnp.einsum(
        "abkcd,kld->abkcl", got_rows, leaf_weight, preferred_element_type=jnp.float32
    )
    mid_held = jnp.einsum(
        "abkcd,kd->abkc", got_rows, mid_weight, preferred_element_type=jnp.float32
    )
    block_lse = jax.nn.logsumexp(scores_held, axis=-1)
    code_float = got_code.astype(jnp.float32)
    labels = jnp.arange(scores_held.shape[-1], dtype=jnp.float32)
    target_hit = (code_float[..., None] == labels).astype(jnp.float32)
    target_held = jnp.sum(scores_held * target_hit, axis=-1)
    back_mid, back_lse, back_target = route_wide((mid_held, block_lse, target_held))
    pair_mid = back_mid.reshape(-1)[slot_of].reshape(rows_here, short_len)
    pair_lse = back_lse.reshape(-1)[slot_of].reshape(rows_here, short_len)
    pair_target = back_target.reshape(-1)[slot_of].reshape(rows_here, short_len)
    mid_totals = jax.nn.logsumexp(pair_mid, axis=1)
    mid_loss = mid_totals - pair_mid[:, 0]
    mid_delta = (jnp.exp(pair_mid - mid_totals[:, None]) - first_slot.astype(jnp.float32)).astype(
        jnp.bfloat16
    )
    leaf_lse = jax.nn.logsumexp(pair_lse, axis=1)
    leaf_loss = leaf_lse - pair_target[:, 0]
    send_delta = (
        jnp.zeros((BLOCKS * CAPB,), jnp.float32)
        .at[slot_of]
        .set(mid_delta.reshape(-1).astype(jnp.float32))
    )
    send_lse = (
        jnp.zeros((BLOCKS * CAPB,), jnp.float32).at[slot_of].set(jnp.repeat(leaf_lse, short_len))
    )
    got_delta, got_lse = route_wide((send_delta.reshape(layout), send_lse.reshape(layout)))
    live_slot = code_float > -1.5
    leaf_delta = jnp.where(
        live_slot[..., None], jnp.exp(scores_held - got_lse[..., None]) - target_hit, 0.0
    ).astype(jnp.bfloat16)
    mid_slots = got_delta.astype(jnp.bfloat16)
    leaf_grad = jnp.einsum(
        "abkcl,abkcd->kld", leaf_delta, got_rows, preferred_element_type=jnp.float32
    )
    mid_grad = jnp.einsum("abkc,abkcd->kd", mid_slots, got_rows, preferred_element_type=jnp.float32)
    pair_back = jnp.einsum(
        "abkcl,kld->abkcd", leaf_delta, leaf_weight, preferred_element_type=jnp.float32
    )
    pair_back = (
        pair_back
        + mid_slots.astype(jnp.float32)[..., None] * mid_weight.astype(jnp.float32)[:, None, :]
    ).astype(jnp.bfloat16)
    returned = route_narrow(pair_back)
    pair_sum = (
        returned.reshape(BLOCKS * CAPB, D)[slot_of]
        .astype(jnp.float32)
        .reshape(rows_here, short_len, D)
        .sum(axis=1)
    )
    query_grad = top_back + pair_sum
    losses = jnp.stack([top_loss, mid_loss, leaf_loss])
    return (query_grad, top_grad, mid_grad, leaf_grad, losses)


LANES = 128
SUB = 8
BF = jnp.bfloat16
F32 = jnp.float32
HIGH = lax.Precision.HIGHEST


def params(mib):
    return pltpu.CompilerParams(vmem_limit_bytes=mib * 1024 * 1024)


def iota(shape, dim):
    return lax.broadcasted_iota(jnp.int32, shape, dim)


def iota_f(shape, dim):
    return iota(shape, dim).astype(F32)


def dot_nn(a, b, precision=None):
    return lax.dot_general(
        a, b, (((1,), (0,)), ((), ())), precision=precision, preferred_element_type=F32
    )


def dot_nt(a, b, precision=None):
    return lax.dot_general(
        a, b, (((1,), (1,)), ((), ())), precision=precision, preferred_element_type=F32
    )


def dot_tn(a, b, precision=None):
    return lax.dot_general(
        a, b, (((0,), (0,)), ((), ())), precision=precision, preferred_element_type=F32
    )


def pack_kernel(
    q_ref, short_ref, slab_ref, leaf_t_ref, top_t_ref, pay_ref, info_ref, own_ref, *, devs, held
):
    rows, width = q_ref.shape
    short_len = short_ref.shape[0]
    clusters = slab_ref.shape[1]
    chunks = width // LANES
    slots = CAPB * held
    cluster_f = iota_f((rows, clusters), 1)
    slab = jnp.broadcast_to(slab_ref[...].astype(F32), (rows, clusters))
    short = short_ref[...].astype(F32)
    short = jnp.concatenate([short, jnp.zeros((rows - short_len, rows), F32)], axis=0).T
    places, hits = [], []
    for j in range(short_len):
        place = jnp.sum(jnp.where(short[:, j : j + 1] == cluster_f, slab, 0.0), axis=1, keepdims=True)
        places.append(place)
        hits.append(jnp.where(place == cluster_f, 1.0, 0.0))
    hit = functools.reduce(lambda a, b: a + b, hits)
    before = jnp.where(iota((rows, rows), 1) < iota((rows, rows), 0), 1.0, 0.0).astype(BF)
    count = dot_nn(before, hit.astype(BF))
    lane = iota((rows, LANES), 1)
    info = jnp.zeros((rows, LANES), F32)
    for j in range(short_len):
        rank = jnp.sum(hits[j] * count, axis=1, keepdims=True)
        info = jnp.where(lane == j, places[j], info)
        info = jnp.where(lane == short_len + j, rank, info)
    info_ref[...] = info
    queries = q_ref[...]
    own_ref[:rows, :] = queries
    top_target = jnp.broadcast_to(top_t_ref[...].astype(F32), (SUB, rows))
    high = jnp.floor(top_target * (1.0 / 256.0))
    code_at = iota((SUB, rows), 0)
    coded = jnp.where(code_at == 0, high, jnp.where(code_at == 1, top_target - 256.0 * high, 0.0))
    own_ref[rows:, :] = jnp.concatenate([coded] * chunks, axis=1).astype(BF)
    target = jnp.broadcast_to(leaf_t_ref[...].astype(F32) + 1.0, (SUB, rows)).astype(BF)
    ones = jnp.ones((SUB, rows), BF)
    table_rows = clusters // LANES
    table = jnp.zeros((CAPB * table_rows, LANES), F32)
    sub = iota((CAPB * table_rows, LANES), 0)
    for r in range(CAPB):
        pick = jnp.where(count == float(r), hit, 0.0)
        chosen = pick.astype(BF)
        first = (pick * hits[0]).astype(BF)
        code = dot_nn(ones, chosen) + dot_nn(target, first)
        for i in range(table_rows):
            part = jnp.broadcast_to(code[0:1, i * LANES : (i + 1) * LANES], table.shape)
            table = jnp.where(sub == r * table_rows + i, part, table)
        got = dot_tn(chosen, queries).astype(BF)
        for c in range(chunks):
            start = c * slots + r * held
            pay_ref[:, start : start + held, :] = got[:, c * LANES : (c + 1) * LANES].reshape(
                devs, held, LANES
            )
    coded = table.astype(BF)
    pay_ref[:, chunks * slots :, :] = jnp.broadcast_to(coded[None], (devs,) + coded.shape)


def halves(source, target, sems):
    half = source.shape[0] // 2
    return [
        pltpu.make_async_copy(
            source.at[pl.ds(n * half, half)], target.at[pl.ds(n * half, half)], sems.at[n]
        )
        for n in range(2)
    ]


def start(copies):
    for copy in copies:
        copy.start()
    return copies


def forward_kernel(
    me_ref, got_ref, leaf_in, mid_ref, rows_out, score_out, stat_ref, code_ref,
    wide_ref, table_ref, leaf_ref, rows_ref, score_ref, leaf_sem, rows_sem, score_sem,
):
    devs, depth, _ = got_ref.shape
    held, labels, width = leaf_ref.shape
    fetches = start(halves(leaf_in, leaf_ref, leaf_sem))
    sends = list(zip(halves(rows_ref, rows_out, rows_sem), halves(score_ref, score_out, score_sem)))
    chunks = width // LANES
    slots = CAPB * held
    body = chunks * slots
    wide_ref[...] = got_ref[:, :body, :].reshape(devs * body, LANES).astype(F32)
    tail = depth - body
    table_ref[...] = got_ref[:, body:, :].astype(F32).reshape(devs * tail, LANES)
    first = me_ref[0] * held
    row_at = first // LANES
    lane_at = first - row_at * LANES
    lane = iota((devs, LANES), 1)
    codes = jnp.zeros((devs, LANES), F32)
    for r in range(CAPB):
        row = table_ref[pl.ds(r * (tail // CAPB) + row_at, devs, stride=tail), :]
        row = pltpu.roll(row, lax.rem(r * held - lane_at + LANES, LANES), 1)
        codes = jnp.where((lane >= r * held) & (lane < (r + 1) * held), row, codes)
    code_ref[...] = codes
    label_f = iota_f((CAPB * devs, labels), 1)
    stats = jnp.zeros((devs, LANES), F32)
    for k in range(held):
        parts = []
        for r in range(CAPB):
            parts.append(
                jnp.concatenate(
                    [
                        wide_ref[pl.ds(c * slots + r * held + k, devs, stride=body), :]
                        for c in range(chunks)
                    ],
                    axis=1,
                )
            )
        full = jnp.concatenate(parts, axis=0)
        rows = full.astype(BF)
        rows_ref[k] = rows
        if k % (held // 2) == 0:
            fetches[k // (held // 2)].wait()
        scores = dot_nt(rows, leaf_ref[k])
        score_ref[k] = scores
        mid = jnp.sum(full * mid_ref[k : k + 1, :].astype(F32), axis=1, keepdims=True)
        peak = jnp.max(scores, axis=1, keepdims=True)
        lse = peak + jnp.log(jnp.sum(jnp.exp(scores - peak), axis=1, keepdims=True))
        code = jnp.concatenate(
            [codes[:, r * held + k : r * held + k + 1] for r in range(CAPB)], axis=0
        )
        target = jnp.sum(jnp.where(code - 2.0 == label_f, scores, 0.0), axis=1, keepdims=True)
        for n, value in enumerate((mid, lse, target)):
            for r in range(CAPB):
                stats = jnp.where(
                    lane == n * slots + r * held + k, value[r * devs : (r + 1) * devs], stats
                )
        if (k + 1) % (held // 2) == 0:
            start(sends[k // (held // 2)])
    stat_ref[...] = stats.reshape(stat_ref.shape)
    for pair in sends:
        for send in pair:
            send.wait()


def middle_kernel(info_ref, stat_ref, out_ref, loss_ref, *, devs, held, short_len):
    rows = info_ref.shape[0]
    slots = CAPB * held
    info = info_ref[...]
    stats = stat_ref[...].reshape(devs, LANES)
    lane = iota_f((rows, LANES), 1)
    dev_f = iota_f((rows, devs), 1)
    owners, spots, mids, lses = [], [], [], []
    for j in range(short_len):
        place = info[:, j : j + 1]
        rank = info[:, short_len + j : short_len + j + 1]
        dev = jnp.floor(place * (1.0 / held))
        spot = place - dev * held + rank * held
        owner = jnp.where(dev == dev_f, 1.0, 0.0)
        values = dot_nn(owner, stats, HIGH)
        owners.append(owner)
        spots.append(spot)
        mids.append(jnp.sum(jnp.where(lane == spot, values, 0.0), axis=1, keepdims=True))
        lses.append(jnp.sum(jnp.where(lane == spot + slots, values, 0.0), axis=1, keepdims=True))
        if j == 0:
            target = jnp.sum(
                jnp.where(lane == spot + 2 * slots, values, 0.0), axis=1, keepdims=True
            )

    def total(columns):
        peak = functools.reduce(jnp.maximum, columns)
        return peak + jnp.log(functools.reduce(lambda a, b: a + b, [jnp.exp(v - peak) for v in columns]))

    mid_total = total(mids)
    leaf_total = total(lses)
    back = []
    for j in range(short_len):
        delta = jnp.exp(mids[j] - mid_total) - (1.0 if j == 0 else 0.0)
        delta = delta.astype(BF).astype(F32)
        back.append(
            jnp.where(
                lane == spots[j], leaf_total, jnp.where(lane == spots[j] + slots, delta, 0.0)
            )
        )
    sent = dot_tn(jnp.concatenate(owners, axis=0), jnp.concatenate(back, axis=0), HIGH)
    out_ref[...] = sent.reshape(out_ref.shape)
    losses = jnp.where(lane == 0.0, mid_total - mids[0], jnp.where(lane == 1.0, leaf_total - target, 0.0))
    loss_ref[...] = losses.T[:SUB, :]


def backward_kernel(
    score_ref, code_ref, norm_ref, leaf_ref, mid_ref, delta_ref, pay_ref, wide_ref
):
    held, pairs, labels = score_ref.shape
    devs = pairs // CAPB
    width = leaf_ref.shape[2]
    chunks = width // LANES
    slots = CAPB * held
    body = chunks * slots
    norms = norm_ref[...].reshape(devs, LANES)
    codes = code_ref[...]
    label_f = iota_f((pairs, labels), 1)

    def column(array, base, k):
        return jnp.concatenate(
            [array[:, base + r * held + k : base + r * held + k + 1] for r in range(CAPB)], axis=0
        )

    for k in range(held):
        code = column(codes, 0, k)
        lse = column(norms, 0, k)
        mid_delta = column(norms, slots, k)
        onehot = jnp.where(code - 2.0 == label_f, 1.0, 0.0)
        delta = jnp.where(code > 0.5, jnp.exp(score_ref[k] - lse) - onehot, 0.0).astype(BF)
        delta_ref[k] = delta
        back = dot_nn(delta, leaf_ref[k]) + mid_delta * mid_ref[k : k + 1, :].astype(F32)
        for r in range(CAPB):
            for c in range(chunks):
                wide_ref[pl.ds(c * slots + r * held + k, devs, stride=body), :] = back[
                    r * devs : (r + 1) * devs, c * LANES : (c + 1) * LANES
                ]
    pay_ref[...] = wide_ref[...].astype(BF).reshape(devs, body, LANES)


def grads_kernel(delta_ref, norm_ref, rows_ref, leaf_grad_ref, mid_grad_ref):
    held, pairs, _ = delta_ref.shape
    devs = pairs // CAPB
    slots = CAPB * held
    norms = norm_ref[...].reshape(devs, LANES)
    for k in range(held):
        rows = rows_ref[k]
        leaf_grad_ref[k] = dot_tn(delta_ref[k], rows)
        mid_delta = jnp.concatenate(
            [norms[:, slots + r * held + k : slots + r * held + k + 1] for r in range(CAPB)], axis=0
        )
        mid_grad_ref[k : k + 1, :] = jnp.sum(mid_delta * rows.astype(F32), axis=0, keepdims=True)


def finish_kernel(info_ref, back_ref, top_ref, out_ref, *, held, short_len):
    rows, width = out_ref.shape
    devs = back_ref.shape[0]
    clusters = devs * held
    chunks = width // LANES
    slots = CAPB * held
    info = info_ref[...]
    cluster_f = iota_f((rows, clusters), 1)
    picks = []
    for r in range(CAPB):
        pick = jnp.zeros((rows, clusters), F32)
        for j in range(short_len):
            place = jnp.where(
                info[:, short_len + j : short_len + j + 1] == float(r), info[:, j : j + 1], -1.0
            )
            pick = jnp.where(place == cluster_f, 1.0, pick)
        picks.append(pick.astype(BF))
    for c in range(chunks):
        total = top_ref[:, c * LANES : (c + 1) * LANES]
        for r in range(CAPB):
            start = c * slots + r * held
            total = total + dot_nn(
                picks[r], back_ref[:, start : start + held, :].reshape(clusters, LANES)
            )
        out_ref[:, c * LANES : (c + 1) * LANES] = total


def top_step(block, target, pieces, weight_held, held_base):
    scores = jnp.concatenate([dot_nt(block, ref[...]) for ref in pieces], axis=1)
    peak = jnp.max(scores, axis=1, keepdims=True)
    total = peak + jnp.log(jnp.sum(jnp.exp(scores - peak), axis=1, keepdims=True))
    mine = dot_nt(block, weight_held)
    held_f = iota_f(mine.shape, 1) + held_base
    delta = (jnp.exp(mine - total) - jnp.where(target == held_f, 1.0, 0.0)).astype(BF)
    return scores, total, dot_tn(delta, block)


def top_column(codes):
    target = codes[0:1, :LANES].astype(F32) * 256.0 + codes[1:2, :LANES].astype(F32)
    return jnp.broadcast_to(target, (LANES, LANES)).T[:, 0:1]


def top_own_kernel(
    where_ref, own_ref, near_ref, y_ref, core_ref, far_ref, column_ref, weight_ref,
    back_ref, part_ref, loss_ref,
):
    rows = own_ref.shape[0] - SUB
    piece = near_ref.shape[0]
    pieces = (near_ref, y_ref, core_ref, far_ref)
    block = own_ref[:rows, :]
    target = top_column(own_ref[rows:, :])
    scores, total, part = top_step(
        block, target, pieces, weight_ref[...], where_ref[0].astype(F32)
    )
    part_ref[...] = part
    hit = jnp.broadcast_to(column_ref[...], scores.shape) == target
    full = (jnp.exp(scores - total) - jnp.where(hit, 1.0, 0.0)).astype(BF)
    back = dot_nn(full[:, :piece], pieces[0][...])
    for n in range(1, len(pieces)):
        back = back + dot_nn(full[:, n * piece : (n + 1) * piece], pieces[n][...])
    back_ref[...] = back
    loss = total - jnp.sum(jnp.where(hit, scores, 0.0), axis=1, keepdims=True)
    loss_ref[...] = jnp.broadcast_to(loss, (rows, LANES)).T[:SUB, :]


def top_more_kernel(
    where_ref, blocks_ref, near_ref, y_ref, core_ref, far_ref, weight_ref, part_ref, out_ref,
    *, first,
):
    count, depth, _ = blocks_ref.shape
    rows = depth - SUB
    numbers = range(first, count)
    block = jnp.concatenate([blocks_ref[n, :rows, :] for n in numbers], axis=0)
    target = jnp.concatenate([top_column(blocks_ref[n, rows:, :]) for n in numbers], axis=0)
    base = where_ref[0].astype(F32)
    pieces = (near_ref, y_ref, core_ref, far_ref)
    part = top_step(block, target, pieces, weight_ref[...], base)[2]
    out_ref[...] = part_ref[...] + part


def spec():
    return pl.BlockSpec(memory_space=pltpu.VMEM)


def call(kernel, outs, ins, scratch=(), scalars=0, far_ins=(), far_outs=(), mib=58):
    far = pl.BlockSpec(memory_space=pltpu.HBM)
    small = pl.BlockSpec(memory_space=pltpu.SMEM)
    listed = isinstance(outs, tuple)
    out_specs = tuple(
        far if n in far_outs else spec() for n in range(len(outs) if listed else 1)
    )
    return pl.pallas_call(
        kernel,
        out_shape=outs,
        in_specs=[
            small if n < scalars else far if n in far_ins else spec() for n in range(len(ins))
        ],
        out_specs=out_specs if listed else out_specs[0],
        scratch_shapes=list(scratch),
        compiler_params=params(mib),
    )(*ins)


def shape(dims, dtype):
    return jax.ShapeDtypeStruct(dims, dtype)


def fits(queries, leaf_weight, shortlist, top_weight, devs, dp_size, label_size):
    rows, width = queries.shape
    held, labels = leaf_weight.shape[:2]
    return (
        rows == LANES
        and labels == LANES
        and width % LANES == 0
        and held % 16 == 0
        and LANES % held == 0
        and 3 * CAPB * held <= LANES
        and CAPB * (devs * held // LANES) % SUB == 0
        and devs % SUB == 0
        and dp_size == 4
        and label_size == 2 * dp_size
        and top_weight.shape[0] % 32 == 0
        and top_weight.shape[0] * label_size <= 65536
        and 2 * shortlist.shape[1] <= LANES
    )


def after(value, first):
    return lax.optimization_barrier((value, first))[0]


def exchange(array):
    return lax.all_to_all(array, ("dp", "label"), split_axis=0, concat_axis=0, tiled=True)


def per_device(
    queries, shortlist, slab_slot, top_target, leaf_target, top_weight, mid_weight, leaf_weight
):
    dp_size = lax.axis_size("dp")
    label_size = lax.axis_size("label")
    devs = dp_size * label_size
    if not fits(queries, leaf_weight, shortlist, top_weight, devs, dp_size, label_size):
        return per_device_any(
            queries, shortlist, slab_slot, top_target, leaf_target, top_weight, mid_weight, leaf_weight
        )
    rows, width = queries.shape
    held, labels = leaf_weight.shape[:2]
    short_len = shortlist.shape[1]
    clusters = devs * held
    chunks = width // LANES
    slots = CAPB * held
    body = chunks * slots
    tail = CAPB * clusters // LANES
    dp_at = lax.axis_index("dp")
    label_at = lax.axis_index("label")
    me = dp_at * label_size + label_at

    steps = label_size // 2
    held_top = top_weight.shape[0]
    flip_x = [(i, i ^ 1) for i in range(label_size)]
    flip_y = [(i, i ^ 2) for i in range(dp_size)]
    flip_core = [(i, i ^ 1) for i in range(dp_size)]

    def along(step):
        return [
            (z * 2 + x, ((z - step) % steps) * 2 + x) for z in range(steps) for x in range(2)
        ]

    shift_z = [
        (d * label_size + z * 2 + x, d * label_size + (z + d + 1) % steps * 2 + x)
        for d in range(dp_size)
        for z in range(steps)
        for x in range(2)
    ]
    w_near = lax.ppermute(top_weight, ("dp", "label"), shift_z)
    me = me.astype(jnp.int32)[None]
    label_base = (label_at * held_top).astype(jnp.int32)[None]
    payload, info, own = call(
        functools.partial(pack_kernel, devs=devs, held=held),
        (
            shape((devs, body + tail, LANES), BF),
            shape((rows, LANES), F32),
            shape((rows + SUB, width), BF),
        ),
        (
            after(queries, (me, label_base)),
            shortlist.T,
            slab_slot[None, :],
            leaf_target[None, :],
            top_target[None, :],
        ),
    )
    got = exchange(payload)
    w_other = lax.ppermute(w_near, "label", flip_x)
    w_own = jnp.concatenate([w_near, w_other])
    w_y = lax.ppermute(w_own, "dp", flip_y)
    w_core = lax.ppermute(w_own, "dp", flip_core)
    z_at, x_at = label_at // 2, label_at % 2
    dp_source = jnp.stack([dp_at, dp_at ^ 2, dp_at ^ 1, dp_at ^ 3])
    source = (z_at - dp_source - 1) % steps * 2
    source = jnp.stack([source + x_at, source + 1 - x_at], axis=1)
    own_column = (source[:, :, None] * held_top + jnp.arange(held_top)).reshape(
        1, label_size * held_top
    )
    sent = after(own, w_near)
    peers = [lax.ppermute(sent, "label", along(n)) for n in range(1, steps)]
    pairs = CAPB * devs
    rows_held, scores, stats, codes = call(
        forward_kernel,
        (
            shape((held, pairs, width), BF),
            shape((held, pairs, labels), F32),
            shape((devs, 1, LANES), F32),
            shape((devs, LANES), F32),
        ),
        (me, got, leaf_weight, mid_weight),
        scratch=(
            pltpu.VMEM((devs * body, LANES), F32),
            pltpu.VMEM((devs * tail, LANES), F32),
            pltpu.VMEM((held, labels, width), BF),
            pltpu.VMEM((held, pairs, width), BF),
            pltpu.VMEM((held, pairs, labels), F32),
            pltpu.SemaphoreType.DMA((2,)),
            pltpu.SemaphoreType.DMA((2,)),
            pltpu.SemaphoreType.DMA((2,)),
        ),
        scalars=1,
        far_ins=(2,),
        far_outs=(0, 1),
    )
    w_y = after(w_y, stats)
    w_far = lax.ppermute(w_y, "dp", flip_core)
    stats_back = exchange(stats)
    norms, pair_losses = call(
        functools.partial(middle_kernel, devs=devs, held=held, short_len=short_len),
        (shape((devs, 1, LANES), F32), shape((SUB, rows), F32)),
        (info, stats_back),
        mib=16,
    )
    norms_held = exchange(norms)
    top_back, top_part, top_loss = call(
        top_own_kernel,
        (
            shape((rows, width), F32),
            shape((held_top, width), F32),
            shape((SUB, rows), F32),
        ),
        (label_base, own, after(w_own, norms), w_y, w_core, w_far, own_column.astype(F32), top_weight),
        scalars=1,
    )
    mine = jnp.stack([sent] + after(peers, top_part))
    other = lax.ppermute(mine, "label", flip_x)
    norms_held = after(norms_held, top_part)
    delta, back = call(
        backward_kernel,
        (shape((held, pairs, labels), BF), shape((devs, body, LANES), BF)),
        (scores, codes, norms_held, leaf_weight, mid_weight),
        scratch=(pltpu.VMEM((devs * body, LANES), F32),),
        mib=24,
    )
    returned = exchange(back)
    top_part = call(
        functools.partial(top_more_kernel, first=1),
        shape((held_top, width), F32),
        (label_base, after(mine, back), w_own, w_y, w_core, w_far, top_weight, top_part),
        scalars=1,
    )
    top_part = call(
        functools.partial(top_more_kernel, first=0),
        shape((held_top, width), F32),
        (label_base, after(other, back), w_own, w_y, w_core, w_far, top_weight, top_part),
        scalars=1,
    )
    losses = jnp.concatenate([top_loss[:1], pair_losses[:2]])
    core = dp_at % 2
    half = held_top // 2
    both = top_part + lax.ppermute(top_part, "dp", flip_core)
    share = lax.dynamic_slice_in_dim(both, core * half, half, 0)
    from_y = lax.ppermute(share, "dp", flip_y)
    leaf_grad, mid_grad = call(
        grads_kernel,
        (shape((held, labels, width), F32), shape((held, width), F32)),
        (delta, norms_held, after(rows_held, (share, losses))),
    )
    share = share + after(from_y, mid_grad)
    rest = lax.ppermute(share, "dp", flip_core)
    top_grad = jnp.concatenate(
        [jnp.where(core == 0, share, rest), jnp.where(core == 0, rest, share)]
    )
    query_grad = call(
        functools.partial(finish_kernel, held=held, short_len=short_len),
        shape((rows, width), F32),
        (info, returned, top_back),
        mib=16,
    )
    return (query_grad, top_grad, mid_grad, leaf_grad, losses)


def solution(mesh):
    in_specs = (
        P(("dp", "label"), None),
        P(("dp", "label"), None),
        P(),
        P(("dp", "label")),
        P(("dp", "label")),
        P("label", None),
        P(("dp", "label"), None),
        P(("dp", "label"), None, None),
    )
    out_specs = (
        P(("dp", "label"), None),
        P("label", None),
        P(("dp", "label"), None),
        P(("dp", "label"), None, None),
        P(None, ("dp", "label")),
    )
    return jax.shard_map(
        per_device, mesh=mesh, in_specs=in_specs, out_specs=out_specs, check_vma=False
    )
```

```python
import functools

import jax
import jax.numpy as jnp
from jax import lax
from jax.experimental import pallas as pl
from jax.experimental.pallas import tpu as pltpu
from jax.sharding import PartitionSpec as P


D = 512
BLOCKS = 512
CAPB = 2


def shortened(array):

    def short(part):
        return part.astype(jnp.bfloat16) if part.dtype == jnp.float32 else part

    return jax.tree.map(short, array)


def route_narrow(payload):
    return jax.tree.map(
        lambda part, own: part.astype(own.dtype),
        lax.all_to_all(
            lax.all_to_all(shortened(payload), "label", split_axis=1, concat_axis=1, tiled=True),
            "dp",
            split_axis=0,
            concat_axis=0,
            tiled=True,
        ),
        payload,
    )


def route_wide(payload):
    return lax.all_to_all(
        lax.all_to_all(payload, "label", split_axis=1, concat_axis=1, tiled=True),
        "dp",
        split_axis=0,
        concat_axis=0,
        tiled=True,
    )


def per_device_any(
    queries, shortlist, slab_slot, top_target, leaf_target, top_weight, mid_weight, leaf_weight
):
    dp_size = lax.axis_size("dp")
    label_size = lax.axis_size("label")
    rows_here = queries.shape[0]
    short_len = shortlist.shape[1]
    block_dev = leaf_weight.shape[0]
    all_rows = lax.all_gather(top_weight, "label", axis=0, tiled=True)
    scores = jnp.dot(queries, all_rows.T, preferred_element_type=jnp.float32)
    totals = jax.nn.logsumexp(scores, axis=1)
    target_hit = top_target[:, None] == jnp.arange(scores.shape[1], dtype=jnp.int32)[None, :]
    top_loss = totals - jnp.sum(jnp.where(target_hit, scores, 0.0), axis=1)
    dscore = (jnp.exp(scores - totals[:, None]) - target_hit.astype(jnp.float32)).astype(
        jnp.bfloat16
    )
    top_back = jnp.dot(dscore, all_rows, preferred_element_type=jnp.float32)
    columns_held = lax.all_to_all(dscore, "label", split_axis=1, concat_axis=0, tiled=True)
    top_part = lax.dot_general(
        columns_held,
        lax.all_gather(queries, "label", axis=0, tiled=True),
        (((0,), (0,)), ((), ())),
        preferred_element_type=jnp.float32,
    )
    top_grad = lax.psum(top_part, "dp")
    position = slab_slot[shortlist].reshape(-1)
    sort_order = jnp.argsort(position, stable=True)
    ranked = position[sort_order]
    run_start = jnp.searchsorted(ranked, ranked, side="left")
    slot_rank = jnp.arange(ranked.shape[0], dtype=jnp.int32) - run_start
    slot_of = jnp.zeros_like(position).at[sort_order].set(ranked * CAPB + slot_rank)
    first_slot = (jnp.arange(short_len, dtype=jnp.int32) == 0)[None, :]
    pair_codes = jnp.where(first_slot, leaf_target[:, None], -1).reshape(-1).astype(jnp.float32)
    layout = (dp_size, label_size, block_dev, CAPB)
    send_rows = (
        jnp.zeros((BLOCKS * CAPB, D), jnp.bfloat16)
        .at[slot_of]
        .set(jnp.repeat(queries, short_len, axis=0))
    )
    send_code = (
        jnp.full((BLOCKS * CAPB,), -2.0, jnp.float32)
        .at[slot_of]
        .set(pair_codes)
        .astype(jnp.bfloat16)
    )
    got_rows, got_code = route_narrow((send_rows.reshape(layout + (D,)), send_code.reshape(layout)))
    scores_held = jnp.einsum(
        "abkcd,kld->abkcl", got_rows, leaf_weight, preferred_element_type=jnp.float32
    )
    mid_held = jnp.einsum(
        "abkcd,kd->abkc", got_rows, mid_weight, preferred_element_type=jnp.float32
    )
    block_lse = jax.nn.logsumexp(scores_held, axis=-1)
    code_float = got_code.astype(jnp.float32)
    labels = jnp.arange(scores_held.shape[-1], dtype=jnp.float32)
    target_hit = (code_float[..., None] == labels).astype(jnp.float32)
    target_held = jnp.sum(scores_held * target_hit, axis=-1)
    back_mid, back_lse, back_target = route_wide((mid_held, block_lse, target_held))
    pair_mid = back_mid.reshape(-1)[slot_of].reshape(rows_here, short_len)
    pair_lse = back_lse.reshape(-1)[slot_of].reshape(rows_here, short_len)
    pair_target = back_target.reshape(-1)[slot_of].reshape(rows_here, short_len)
    mid_totals = jax.nn.logsumexp(pair_mid, axis=1)
    mid_loss = mid_totals - pair_mid[:, 0]
    mid_delta = (jnp.exp(pair_mid - mid_totals[:, None]) - first_slot.astype(jnp.float32)).astype(
        jnp.bfloat16
    )
    leaf_lse = jax.nn.logsumexp(pair_lse, axis=1)
    leaf_loss = leaf_lse - pair_target[:, 0]
    send_delta = (
        jnp.zeros((BLOCKS * CAPB,), jnp.float32)
        .at[slot_of]
        .set(mid_delta.reshape(-1).astype(jnp.float32))
    )
    send_lse = (
        jnp.zeros((BLOCKS * CAPB,), jnp.float32).at[slot_of].set(jnp.repeat(leaf_lse, short_len))
    )
    got_delta, got_lse = route_wide((send_delta.reshape(layout), send_lse.reshape(layout)))
    live_slot = code_float > -1.5
    leaf_delta = jnp.where(
        live_slot[..., None], jnp.exp(scores_held - got_lse[..., None]) - target_hit, 0.0
    ).astype(jnp.bfloat16)
    mid_slots = got_delta.astype(jnp.bfloat16)
    leaf_grad = jnp.einsum(
        "abkcl,abkcd->kld", leaf_delta, got_rows, preferred_element_type=jnp.float32
    )
    mid_grad = jnp.einsum("abkc,abkcd->kd", mid_slots, got_rows, preferred_element_type=jnp.float32)
    pair_back = jnp.einsum(
        "abkcl,kld->abkcd", leaf_delta, leaf_weight, preferred_element_type=jnp.float32
    )
    pair_back = (
        pair_back
        + mid_slots.astype(jnp.float32)[..., None] * mid_weight.astype(jnp.float32)[:, None, :]
    ).astype(jnp.bfloat16)
    returned = route_narrow(pair_back)
    pair_sum = (
        returned.reshape(BLOCKS * CAPB, D)[slot_of]
        .astype(jnp.float32)
        .reshape(rows_here, short_len, D)
        .sum(axis=1)
    )
    query_grad = top_back + pair_sum
    losses = jnp.stack([top_loss, mid_loss, leaf_loss])
    return (query_grad, top_grad, mid_grad, leaf_grad, losses)


LANES = 128
SUB = 8
BF = jnp.bfloat16
F32 = jnp.float32
HIGH = lax.Precision.HIGHEST


def params(mib):
    return pltpu.CompilerParams(vmem_limit_bytes=mib * 1024 * 1024)


def iota(shape, dim):
    return lax.broadcasted_iota(jnp.int32, shape, dim)


def iota_f(shape, dim):
    return iota(shape, dim).astype(F32)


def dot_nn(a, b, precision=None):
    return lax.dot_general(
        a, b, (((1,), (0,)), ((), ())), precision=precision, preferred_element_type=F32
    )


def dot_nt(a, b, precision=None):
    return lax.dot_general(
        a, b, (((1,), (1,)), ((), ())), precision=precision, preferred_element_type=F32
    )


def dot_tn(a, b, precision=None):
    return lax.dot_general(
        a, b, (((0,), (0,)), ((), ())), precision=precision, preferred_element_type=F32
    )


def pack_kernel(
    q_ref, short_ref, slab_ref, leaf_t_ref, top_t_ref, pay_ref, info_ref, own_ref, *, devs, held
):
    rows, width = q_ref.shape
    short_len = short_ref.shape[0]
    clusters = slab_ref.shape[1]
    chunks = width // LANES
    slots = CAPB * held
    cluster_f = iota_f((rows, clusters), 1)
    slab = jnp.broadcast_to(slab_ref[...].astype(F32), (rows, clusters))
    short = short_ref[...].astype(F32)
    short = jnp.concatenate([short, jnp.zeros((rows - short_len, rows), F32)], axis=0).T
    places, hits = [], []
    for j in range(short_len):
        place = jnp.sum(jnp.where(short[:, j : j + 1] == cluster_f, slab, 0.0), axis=1, keepdims=True)
        places.append(place)
        hits.append(jnp.where(place == cluster_f, 1.0, 0.0))
    hit = functools.reduce(lambda a, b: a + b, hits)
    before = jnp.where(iota((rows, rows), 1) < iota((rows, rows), 0), 1.0, 0.0).astype(BF)
    count = dot_nn(before, hit.astype(BF))
    lane = iota((rows, LANES), 1)
    info = jnp.zeros((rows, LANES), F32)
    for j in range(short_len):
        rank = jnp.sum(hits[j] * count, axis=1, keepdims=True)
        info = jnp.where(lane == j, places[j], info)
        info = jnp.where(lane == short_len + j, rank, info)
    info_ref[...] = info
    queries = q_ref[...]
    own_ref[:rows, :] = queries
    top_target = jnp.broadcast_to(top_t_ref[...].astype(F32), (SUB, rows))
    high = jnp.floor(top_target * (1.0 / 256.0))
    code_at = iota((SUB, rows), 0)
    coded = jnp.where(code_at == 0, high, jnp.where(code_at == 1, top_target - 256.0 * high, 0.0))
    own_ref[rows:, :] = jnp.concatenate([coded] * chunks, axis=1).astype(BF)
    target = jnp.broadcast_to(leaf_t_ref[...].astype(F32) + 1.0, (SUB, rows)).astype(BF)
    ones = jnp.ones((SUB, rows), BF)
    table_rows = clusters // LANES
    table = jnp.zeros((CAPB * table_rows, LANES), F32)
    sub = iota((CAPB * table_rows, LANES), 0)
    for r in range(CAPB):
        pick = jnp.where(count == float(r), hit, 0.0)
        chosen = pick.astype(BF)
        first = (pick * hits[0]).astype(BF)
        code = dot_nn(ones, chosen) + dot_nn(target, first)
        for i in range(table_rows):
            part = jnp.broadcast_to(code[0:1, i * LANES : (i + 1) * LANES], table.shape)
            table = jnp.where(sub == r * table_rows + i, part, table)
        got = dot_tn(chosen, queries).astype(BF)
        for c in range(chunks):
            start = c * slots + r * held
            pay_ref[:, start : start + held, :] = got[:, c * LANES : (c + 1) * LANES].reshape(
                devs, held, LANES
            )
    coded = table.astype(BF)
    pay_ref[:, chunks * slots :, :] = jnp.broadcast_to(coded[None], (devs,) + coded.shape)


def halves(source, target, sems):
    half = source.shape[0] // 2
    return [
        pltpu.make_async_copy(
            source.at[pl.ds(n * half, half)], target.at[pl.ds(n * half, half)], sems.at[n]
        )
        for n in range(2)
    ]


def start(copies):
    for copy in copies:
        copy.start()
    return copies


def cluster_rows(wide_ref, k, devs, held, chunks):
    slots = CAPB * held
    return jnp.concatenate(
        [
            jnp.concatenate(
                [
                    wide_ref[pl.ds(c * slots + r * held + k, devs, stride=chunks * slots), :]
                    for c in range(chunks)
                ],
                axis=1,
            )
            for r in range(CAPB)
        ],
        axis=0,
    )


def forward_kernel(
    me_ref, got_ref, leaf_in, mid_ref, score_ref, stat_ref, code_ref,
    wide_ref, table_ref, leaf_ref, leaf_sem,
):
    devs, depth, _ = got_ref.shape
    held, labels, width = leaf_ref.shape
    fetches = start(halves(leaf_in, leaf_ref, leaf_sem))
    chunks = width // LANES
    slots = CAPB * held
    body = chunks * slots
    wide_ref[...] = got_ref[:, :body, :].reshape(devs * body, LANES).astype(F32)
    tail = depth - body
    table_ref[...] = got_ref[:, body:, :].astype(F32).reshape(devs * tail, LANES)
    first = me_ref[0] * held
    row_at = first // LANES
    lane_at = first - row_at * LANES
    lane = iota((devs, LANES), 1)
    codes = jnp.zeros((devs, LANES), F32)
    for r in range(CAPB):
        row = table_ref[pl.ds(r * (tail // CAPB) + row_at, devs, stride=tail), :]
        row = pltpu.roll(row, lax.rem(r * held - lane_at + LANES, LANES), 1)
        codes = jnp.where((lane >= r * held) & (lane < (r + 1) * held), row, codes)
    code_ref[...] = codes
    label_f = iota_f((CAPB * devs, labels), 1)
    stats = jnp.zeros((devs, LANES), F32)
    for k in range(held):
        full = cluster_rows(wide_ref, k, devs, held, chunks)
        rows = full.astype(BF)
        if k % (held // 2) == 0:
            fetches[k // (held // 2)].wait()
        scores = dot_nt(rows, leaf_ref[k])
        score_ref[k] = scores
        mid = jnp.sum(full * mid_ref[k : k + 1, :].astype(F32), axis=1, keepdims=True)
        peak = jnp.max(scores, axis=1, keepdims=True)
        lse = peak + jnp.log(jnp.sum(jnp.exp(scores - peak), axis=1, keepdims=True))
        code = jnp.concatenate(
            [codes[:, r * held + k : r * held + k + 1] for r in range(CAPB)], axis=0
        )
        target = jnp.sum(jnp.where(code - 2.0 == label_f, scores, 0.0), axis=1, keepdims=True)
        for n, value in enumerate((mid, lse, target)):
            for r in range(CAPB):
                stats = jnp.where(
                    lane == n * slots + r * held + k, value[r * devs : (r + 1) * devs], stats
                )
    stat_ref[...] = stats.reshape(stat_ref.shape)


def middle_kernel(info_ref, stat_ref, out_ref, loss_ref, *, devs, held, short_len):
    rows = info_ref.shape[0]
    slots = CAPB * held
    info = info_ref[...]
    stats = stat_ref[...].reshape(devs, LANES)
    lane = iota_f((rows, LANES), 1)
    dev_f = iota_f((rows, devs), 1)
    owners, spots, mids, lses = [], [], [], []
    for j in range(short_len):
        place = info[:, j : j + 1]
        rank = info[:, short_len + j : short_len + j + 1]
        dev = jnp.floor(place * (1.0 / held))
        spot = place - dev * held + rank * held
        owner = jnp.where(dev == dev_f, 1.0, 0.0)
        values = dot_nn(owner, stats, HIGH)
        owners.append(owner)
        spots.append(spot)
        mids.append(jnp.sum(jnp.where(lane == spot, values, 0.0), axis=1, keepdims=True))
        lses.append(jnp.sum(jnp.where(lane == spot + slots, values, 0.0), axis=1, keepdims=True))
        if j == 0:
            target = jnp.sum(
                jnp.where(lane == spot + 2 * slots, values, 0.0), axis=1, keepdims=True
            )

    def total(columns):
        peak = functools.reduce(jnp.maximum, columns)
        return peak + jnp.log(functools.reduce(lambda a, b: a + b, [jnp.exp(v - peak) for v in columns]))

    mid_total = total(mids)
    leaf_total = total(lses)
    back = []
    for j in range(short_len):
        delta = jnp.exp(mids[j] - mid_total) - (1.0 if j == 0 else 0.0)
        delta = delta.astype(BF).astype(F32)
        back.append(
            jnp.where(
                lane == spots[j], leaf_total, jnp.where(lane == spots[j] + slots, delta, 0.0)
            )
        )
    sent = dot_tn(jnp.concatenate(owners, axis=0), jnp.concatenate(back, axis=0), HIGH)
    out_ref[...] = sent.reshape(out_ref.shape)
    losses = jnp.where(lane == 0.0, mid_total - mids[0], jnp.where(lane == 1.0, leaf_total - target, 0.0))
    loss_ref[...] = losses.T[:SUB, :]


def backward_kernel(
    score_ref, code_ref, norm_ref, leaf_ref, mid_ref, delta_ref, pay_ref, wide_ref
):
    held, pairs, labels = score_ref.shape
    devs = pairs // CAPB
    width = leaf_ref.shape[2]
    chunks = width // LANES
    slots = CAPB * held
    body = chunks * slots
    norms = norm_ref[...].reshape(devs, LANES)
    codes = code_ref[...]
    label_f = iota_f((pairs, labels), 1)

    def column(array, base, k):
        return jnp.concatenate(
            [array[:, base + r * held + k : base + r * held + k + 1] for r in range(CAPB)], axis=0
        )

    for k in range(held):
        code = column(codes, 0, k)
        lse = column(norms, 0, k)
        mid_delta = column(norms, slots, k)
        onehot = jnp.where(code - 2.0 == label_f, 1.0, 0.0)
        delta = jnp.where(code > 0.5, jnp.exp(score_ref[k] - lse) - onehot, 0.0).astype(BF)
        delta_ref[k] = delta
        back = dot_nn(delta, leaf_ref[k]) + mid_delta * mid_ref[k : k + 1, :].astype(F32)
        for r in range(CAPB):
            for c in range(chunks):
                wide_ref[pl.ds(c * slots + r * held + k, devs, stride=body), :] = back[
                    r * devs : (r + 1) * devs, c * LANES : (c + 1) * LANES
                ]
    pay_ref[...] = wide_ref[...].astype(BF).reshape(devs, body, LANES)


def grads_kernel(delta_ref, norm_ref, got_ref, leaf_grad_ref, mid_grad_ref, wide_ref):
    held, pairs, _ = delta_ref.shape
    devs = pairs // CAPB
    slots = CAPB * held
    chunks = leaf_grad_ref.shape[2] // LANES
    body = chunks * slots
    wide_ref[...] = got_ref[:, :body, :].reshape(devs * body, LANES).astype(F32)
    norms = norm_ref[...].reshape(devs, LANES)
    for k in range(held):
        full = cluster_rows(wide_ref, k, devs, held, chunks)
        leaf_grad_ref[k] = dot_tn(delta_ref[k], full.astype(BF))
        mid_delta = jnp.concatenate(
            [norms[:, slots + r * held + k : slots + r * held + k + 1] for r in range(CAPB)], axis=0
        )
        mid_grad_ref[k : k + 1, :] = jnp.sum(mid_delta * full, axis=0, keepdims=True)


def finish_kernel(
    info_ref, back_ref, top_ref, top_loss_ref, pair_loss_ref, out_ref, loss_ref, *, held, short_len
):
    loss_ref[0:1, :] = top_loss_ref[0:1, :]
    loss_ref[1:3, :] = pair_loss_ref[0:2, :]
    rows, width = out_ref.shape
    devs = back_ref.shape[0]
    clusters = devs * held
    chunks = width // LANES
    slots = CAPB * held
    info = info_ref[...]
    cluster_f = iota_f((rows, clusters), 1)
    picks = []
    for r in range(CAPB):
        pick = jnp.zeros((rows, clusters), F32)
        for j in range(short_len):
            place = jnp.where(
                info[:, short_len + j : short_len + j + 1] == float(r), info[:, j : j + 1], -1.0
            )
            pick = jnp.where(place == cluster_f, 1.0, pick)
        picks.append(pick.astype(BF))
    for c in range(chunks):
        total = top_ref[:, c * LANES : (c + 1) * LANES]
        for r in range(CAPB):
            start = c * slots + r * held
            total = total + dot_nn(
                picks[r], back_ref[:, start : start + held, :].reshape(clusters, LANES)
            )
        out_ref[:, c * LANES : (c + 1) * LANES] = total


def top_step(block, target, pieces, weight_held, held_base):
    scores = jnp.concatenate([dot_nt(block, ref[...]) for ref in pieces], axis=1)
    peak = jnp.max(scores, axis=1, keepdims=True)
    total = peak + jnp.log(jnp.sum(jnp.exp(scores - peak), axis=1, keepdims=True))
    mine = dot_nt(block, weight_held)
    held_f = iota_f(mine.shape, 1) + held_base
    delta = (jnp.exp(mine - total) - jnp.where(target == held_f, 1.0, 0.0)).astype(BF)
    return scores, total, dot_tn(delta, block)


def top_column(codes):
    target = codes[0:1, :LANES].astype(F32) * 256.0 + codes[1:2, :LANES].astype(F32)
    return jnp.broadcast_to(target, (LANES, LANES)).T[:, 0:1]


def own_columns(me, dims, label_size, held_top):
    steps = label_size // 2

    def split(value, size):
        high = jnp.floor((value + 0.5) * (1.0 / size))
        return high, value - high * size

    def flip(bit, other):
        return bit + other - 2.0 * bit * other

    dp_at, label_at = split(jnp.full(dims, me, jnp.int32).astype(F32), label_size)
    y_at, core_at = split(dp_at, 2)
    z_at, x_at = split(label_at, 2)
    part, rest = split(iota_f(dims, 1), 2 * held_top)
    side, row = split(rest, held_top)
    core_bit, y_bit = split(part, 2)
    dp_from = flip(y_at, y_bit) * 2.0 + flip(core_at, core_bit)
    z_from = z_at - dp_from - 1.0
    z_from = jnp.where(z_from < 0.0, z_from + steps, z_from)
    return (z_from * 2.0 + flip(x_at, side)) * held_top + row


def top_own_kernel(
    where_ref, me_ref, own_ref, near_ref, y_ref, core_ref, far_ref, weight_ref,
    back_ref, part_ref, loss_ref, *, label_size,
):
    rows = own_ref.shape[0] - SUB
    piece = near_ref.shape[0]
    pieces = (near_ref, y_ref, core_ref, far_ref)
    block = own_ref[:rows, :]
    target = top_column(own_ref[rows:, :])
    scores, total, part = top_step(
        block, target, pieces, weight_ref[...], where_ref[0].astype(F32)
    )
    part_ref[...] = part
    column = own_columns(me_ref[0], (SUB, scores.shape[1]), label_size, weight_ref.shape[0])
    hit = jnp.broadcast_to(column[0:1, :], scores.shape) == target
    full = (jnp.exp(scores - total) - jnp.where(hit, 1.0, 0.0)).astype(BF)
    back = dot_nn(full[:, :piece], pieces[0][...])
    for n in range(1, len(pieces)):
        back = back + dot_nn(full[:, n * piece : (n + 1) * piece], pieces[n][...])
    back_ref[...] = back
    loss = total - jnp.sum(jnp.where(hit, scores, 0.0), axis=1, keepdims=True)
    loss_ref[...] = jnp.broadcast_to(loss, (rows, LANES)).T[:SUB, :]


def top_blocks(where_ref, blocks_ref, pieces, weight_ref, first):
    count, depth, _ = blocks_ref.shape
    rows = depth - SUB
    numbers = range(first, count)
    block = jnp.concatenate([blocks_ref[n, :rows, :] for n in numbers], axis=0)
    target = jnp.concatenate([top_column(blocks_ref[n, rows:, :]) for n in numbers], axis=0)
    return top_step(block, target, pieces, weight_ref[...], where_ref[0].astype(F32))[2]


def top_near_kernel(
    where_ref, blocks_ref, near_ref, y_ref, core_ref, far_ref, weight_ref, part_ref, out_ref
):
    pieces = (near_ref, y_ref, core_ref, far_ref)
    out_ref[...] = part_ref[...] + top_blocks(where_ref, blocks_ref, pieces, weight_ref, 1)


def top_far_kernel(
    where_ref, me_ref, blocks_ref, near_ref, y_ref, core_ref, far_ref, weight_ref, part_ref,
    kept_ref, given_ref, sum_ref, *, label_size,
):
    pieces = (near_ref, y_ref, core_ref, far_ref)
    sum_ref[...] = part_ref[...] + top_blocks(where_ref, blocks_ref, pieces, weight_ref, 0)
    half = kept_ref.shape[0]
    core = lax.rem(lax.div(me_ref[0], label_size), 2)
    kept_ref[...] = sum_ref[pl.ds(pl.multiple_of(core * half, SUB), half), :]
    given_ref[...] = sum_ref[pl.ds(pl.multiple_of((1 - core) * half, SUB), half), :]


def spec():
    return pl.BlockSpec(memory_space=pltpu.VMEM)


def call(kernel, outs, ins, scratch=(), scalars=0, far_ins=(), far_outs=(), mib=58):
    far = pl.BlockSpec(memory_space=pltpu.HBM)
    small = pl.BlockSpec(memory_space=pltpu.SMEM)
    listed = isinstance(outs, tuple)
    out_specs = tuple(
        far if n in far_outs else spec() for n in range(len(outs) if listed else 1)
    )
    return pl.pallas_call(
        kernel,
        out_shape=outs,
        in_specs=[
            small if n < scalars else far if n in far_ins else spec() for n in range(len(ins))
        ],
        out_specs=out_specs if listed else out_specs[0],
        scratch_shapes=list(scratch),
        compiler_params=params(mib),
    )(*ins)


def shape(dims, dtype):
    return jax.ShapeDtypeStruct(dims, dtype)


def fits(queries, leaf_weight, shortlist, top_weight, devs, dp_size, label_size):
    rows, width = queries.shape
    held, labels = leaf_weight.shape[:2]
    return (
        rows == LANES
        and labels == LANES
        and width % LANES == 0
        and held % 16 == 0
        and LANES % held == 0
        and 3 * CAPB * held <= LANES
        and CAPB * (devs * held // LANES) % SUB == 0
        and devs % SUB == 0
        and dp_size == 4
        and label_size == 2 * dp_size
        and top_weight.shape[0] % 32 == 0
        and top_weight.shape[0] * label_size <= 65536
        and 2 * shortlist.shape[1] <= LANES
    )


def after(value, first):
    return lax.optimization_barrier((value, first))[0]


def exchange(array):
    return lax.all_to_all(array, ("dp", "label"), split_axis=0, concat_axis=0, tiled=True)


def per_device(
    queries, shortlist, slab_slot, top_target, leaf_target, top_weight, mid_weight, leaf_weight
):
    dp_size = lax.axis_size("dp")
    label_size = lax.axis_size("label")
    devs = dp_size * label_size
    if not fits(queries, leaf_weight, shortlist, top_weight, devs, dp_size, label_size):
        return per_device_any(
            queries, shortlist, slab_slot, top_target, leaf_target, top_weight, mid_weight, leaf_weight
        )
    rows, width = queries.shape
    held, labels = leaf_weight.shape[:2]
    short_len = shortlist.shape[1]
    clusters = devs * held
    chunks = width // LANES
    slots = CAPB * held
    body = chunks * slots
    tail = CAPB * clusters // LANES
    dp_at = lax.axis_index("dp")
    label_at = lax.axis_index("label")
    me = dp_at * label_size + label_at

    steps = label_size // 2
    held_top = top_weight.shape[0]
    flip_x = [(i, i ^ 1) for i in range(label_size)]
    flip_y = [(i, i ^ 2) for i in range(dp_size)]
    flip_core = [(i, i ^ 1) for i in range(dp_size)]

    def along(step):
        return [
            (z * 2 + x, ((z - step) % steps) * 2 + x) for z in range(steps) for x in range(2)
        ]

    shift_z = [
        (d * label_size + z * 2 + x, d * label_size + (z + d + 1) % steps * 2 + x)
        for d in range(dp_size)
        for z in range(steps)
        for x in range(2)
    ]
    w_near = lax.ppermute(top_weight, ("dp", "label"), shift_z)
    me = me.astype(jnp.int32)[None]
    label_base = (label_at * held_top).astype(jnp.int32)[None]
    payload, info, own = call(
        functools.partial(pack_kernel, devs=devs, held=held),
        (
            shape((devs, body + tail, LANES), BF),
            shape((rows, LANES), F32),
            shape((rows + SUB, width), BF),
        ),
        (
            after(queries, (me, label_base)),
            shortlist.T,
            slab_slot[None, :],
            leaf_target[None, :],
            top_target[None, :],
        ),
    )
    got = exchange(payload)
    w_other = lax.ppermute(w_near, "label", flip_x)
    w_own = jnp.concatenate([w_near, w_other])
    w_y = lax.ppermute(w_own, "dp", flip_y)
    w_core = lax.ppermute(w_own, "dp", flip_core)
    sent = after(own, w_near)
    peers = [lax.ppermute(sent, "label", along(n)) for n in range(1, steps)]
    pairs = CAPB * devs
    scores, stats, codes = call(
        forward_kernel,
        (
            shape((held, pairs, labels), F32),
            shape((devs, 1, LANES), F32),
            shape((devs, LANES), F32),
        ),
        (me, got, leaf_weight, mid_weight),
        scratch=(
            pltpu.VMEM((devs * body, LANES), F32),
            pltpu.VMEM((devs * tail, LANES), F32),
            pltpu.VMEM((held, labels, width), BF),
            pltpu.SemaphoreType.DMA((2,)),
        ),
        scalars=1,
        far_ins=(2,),
        mib=50,
    )
    w_y = after(w_y, stats)
    w_far = lax.ppermute(w_y, "dp", flip_core)
    stats_back = exchange(stats)
    norms, pair_losses = call(
        functools.partial(middle_kernel, devs=devs, held=held, short_len=short_len),
        (shape((devs, 1, LANES), F32), shape((SUB, rows), F32)),
        (info, stats_back),
        mib=16,
    )
    norms_held = exchange(norms)
    top_back, top_part, top_loss = call(
        functools.partial(top_own_kernel, label_size=label_size),
        (
            shape((rows, width), F32),
            shape((held_top, width), F32),
            shape((SUB, rows), F32),
        ),
        (label_base, me, own, after(w_own, norms), w_y, w_core, w_far, top_weight),
        scalars=2,
    )
    mine = jnp.stack([sent] + after(peers, top_part))
    other = lax.ppermute(mine, "label", flip_x)
    norms_held = after(norms_held, top_part)
    delta, back = call(
        backward_kernel,
        (shape((held, pairs, labels), BF), shape((devs, body, LANES), BF)),
        (scores, codes, norms_held, leaf_weight, mid_weight),
        scratch=(pltpu.VMEM((devs * body, LANES), F32),),
        mib=24,
    )
    returned = exchange(back)
    top_part = call(
        top_near_kernel,
        shape((held_top, width), F32),
        (label_base, after(mine, back), w_own, w_y, w_core, w_far, top_weight, top_part),
        scalars=1,
    )
    kept, given = call(
        functools.partial(top_far_kernel, label_size=label_size),
        (shape((held_top // 2, width), F32), shape((held_top // 2, width), F32)),
        (label_base, me, after(other, back), w_own, w_y, w_core, w_far, top_weight, top_part),
        scalars=2,
        scratch=(pltpu.VMEM((held_top, width), F32),),
    )
    core = dp_at % 2
    share = kept + lax.ppermute(given, "dp", flip_core)
    from_y = lax.ppermute(share, "dp", flip_y)
    leaf_grad, mid_grad = call(
        grads_kernel,
        (shape((held, labels, width), F32), shape((held, width), F32)),
        (delta, norms_held, after(got, share)),
        scratch=(pltpu.VMEM((devs * body, LANES), F32),),
    )
    share = share + after(from_y, mid_grad)
    rest = lax.ppermute(share, "dp", flip_core)
    top_grad = jnp.concatenate(
        [jnp.where(core == 0, share, rest), jnp.where(core == 0, rest, share)]
    )
    query_grad, losses = call(
        functools.partial(finish_kernel, held=held, short_len=short_len),
        (shape((rows, width), F32), shape((3, rows), F32)),
        (info, returned, top_back, top_loss, pair_losses),
        mib=16,
    )
    return (query_grad, top_grad, mid_grad, leaf_grad, losses)


def solution(mesh):
    in_specs = (
        P(("dp", "label"), None),
        P(("dp", "label"), None),
        P(),
        P(("dp", "label")),
        P(("dp", "label")),
        P("label", None),
        P(("dp", "label"), None),
        P(("dp", "label"), None, None),
    )
    out_specs = (
        P(("dp", "label"), None),
        P("label", None),
        P(("dp", "label"), None),
        P(("dp", "label"), None, None),
        P(None, ("dp", "label")),
    )
    return jax.shard_map(
        per_device, mesh=mesh, in_specs=in_specs, out_specs=out_specs, check_vma=False
    )
```

```python
import functools

import jax
import jax.numpy as jnp
from jax import lax
from jax.experimental import pallas as pl
from jax.experimental.pallas import tpu as pltpu
from jax.sharding import PartitionSpec as P


D = 512
BLOCKS = 512
CAPB = 2


def shortened(array):

    def short(part):
        return part.astype(jnp.bfloat16) if part.dtype == jnp.float32 else part

    return jax.tree.map(short, array)


def route_narrow(payload):
    return jax.tree.map(
        lambda part, own: part.astype(own.dtype),
        lax.all_to_all(
            lax.all_to_all(shortened(payload), "label", split_axis=1, concat_axis=1, tiled=True),
            "dp",
            split_axis=0,
            concat_axis=0,
            tiled=True,
        ),
        payload,
    )


def route_wide(payload):
    return lax.all_to_all(
        lax.all_to_all(payload, "label", split_axis=1, concat_axis=1, tiled=True),
        "dp",
        split_axis=0,
        concat_axis=0,
        tiled=True,
    )


def per_device_any(
    queries, shortlist, slab_slot, top_target, leaf_target, top_weight, mid_weight, leaf_weight
):
    dp_size = lax.axis_size("dp")
    label_size = lax.axis_size("label")
    rows_here = queries.shape[0]
    short_len = shortlist.shape[1]
    block_dev = leaf_weight.shape[0]
    all_rows = lax.all_gather(top_weight, "label", axis=0, tiled=True)
    scores = jnp.dot(queries, all_rows.T, preferred_element_type=jnp.float32)
    totals = jax.nn.logsumexp(scores, axis=1)
    target_hit = top_target[:, None] == jnp.arange(scores.shape[1], dtype=jnp.int32)[None, :]
    top_loss = totals - jnp.sum(jnp.where(target_hit, scores, 0.0), axis=1)
    dscore = (jnp.exp(scores - totals[:, None]) - target_hit.astype(jnp.float32)).astype(
        jnp.bfloat16
    )
    top_back = jnp.dot(dscore, all_rows, preferred_element_type=jnp.float32)
    columns_held = lax.all_to_all(dscore, "label", split_axis=1, concat_axis=0, tiled=True)
    top_part = lax.dot_general(
        columns_held,
        lax.all_gather(queries, "label", axis=0, tiled=True),
        (((0,), (0,)), ((), ())),
        preferred_element_type=jnp.float32,
    )
    top_grad = lax.psum(top_part, "dp")
    position = slab_slot[shortlist].reshape(-1)
    sort_order = jnp.argsort(position, stable=True)
    ranked = position[sort_order]
    run_start = jnp.searchsorted(ranked, ranked, side="left")
    slot_rank = jnp.arange(ranked.shape[0], dtype=jnp.int32) - run_start
    slot_of = jnp.zeros_like(position).at[sort_order].set(ranked * CAPB + slot_rank)
    first_slot = (jnp.arange(short_len, dtype=jnp.int32) == 0)[None, :]
    pair_codes = jnp.where(first_slot, leaf_target[:, None], -1).reshape(-1).astype(jnp.float32)
    layout = (dp_size, label_size, block_dev, CAPB)
    send_rows = (
        jnp.zeros((BLOCKS * CAPB, D), jnp.bfloat16)
        .at[slot_of]
        .set(jnp.repeat(queries, short_len, axis=0))
    )
    send_code = (
        jnp.full((BLOCKS * CAPB,), -2.0, jnp.float32)
        .at[slot_of]
        .set(pair_codes)
        .astype(jnp.bfloat16)
    )
    got_rows, got_code = route_narrow((send_rows.reshape(layout + (D,)), send_code.reshape(layout)))
    scores_held = jnp.einsum(
        "abkcd,kld->abkcl", got_rows, leaf_weight, preferred_element_type=jnp.float32
    )
    mid_held = jnp.einsum(
        "abkcd,kd->abkc", got_rows, mid_weight, preferred_element_type=jnp.float32
    )
    block_lse = jax.nn.logsumexp(scores_held, axis=-1)
    code_float = got_code.astype(jnp.float32)
    labels = jnp.arange(scores_held.shape[-1], dtype=jnp.float32)
    target_hit = (code_float[..., None] == labels).astype(jnp.float32)
    target_held = jnp.sum(scores_held * target_hit, axis=-1)
    back_mid, back_lse, back_target = route_wide((mid_held, block_lse, target_held))
    pair_mid = back_mid.reshape(-1)[slot_of].reshape(rows_here, short_len)
    pair_lse = back_lse.reshape(-1)[slot_of].reshape(rows_here, short_len)
    pair_target = back_target.reshape(-1)[slot_of].reshape(rows_here, short_len)
    mid_totals = jax.nn.logsumexp(pair_mid, axis=1)
    mid_loss = mid_totals - pair_mid[:, 0]
    mid_delta = (jnp.exp(pair_mid - mid_totals[:, None]) - first_slot.astype(jnp.float32)).astype(
        jnp.bfloat16
    )
    leaf_lse = jax.nn.logsumexp(pair_lse, axis=1)
    leaf_loss = leaf_lse - pair_target[:, 0]
    send_delta = (
        jnp.zeros((BLOCKS * CAPB,), jnp.float32)
        .at[slot_of]
        .set(mid_delta.reshape(-1).astype(jnp.float32))
    )
    send_lse = (
        jnp.zeros((BLOCKS * CAPB,), jnp.float32).at[slot_of].set(jnp.repeat(leaf_lse, short_len))
    )
    got_delta, got_lse = route_wide((send_delta.reshape(layout), send_lse.reshape(layout)))
    live_slot = code_float > -1.5
    leaf_delta = jnp.where(
        live_slot[..., None], jnp.exp(scores_held - got_lse[..., None]) - target_hit, 0.0
    ).astype(jnp.bfloat16)
    mid_slots = got_delta.astype(jnp.bfloat16)
    leaf_grad = jnp.einsum(
        "abkcl,abkcd->kld", leaf_delta, got_rows, preferred_element_type=jnp.float32
    )
    mid_grad = jnp.einsum("abkc,abkcd->kd", mid_slots, got_rows, preferred_element_type=jnp.float32)
    pair_back = jnp.einsum(
        "abkcl,kld->abkcd", leaf_delta, leaf_weight, preferred_element_type=jnp.float32
    )
    pair_back = (
        pair_back
        + mid_slots.astype(jnp.float32)[..., None] * mid_weight.astype(jnp.float32)[:, None, :]
    ).astype(jnp.bfloat16)
    returned = route_narrow(pair_back)
    pair_sum = (
        returned.reshape(BLOCKS * CAPB, D)[slot_of]
        .astype(jnp.float32)
        .reshape(rows_here, short_len, D)
        .sum(axis=1)
    )
    query_grad = top_back + pair_sum
    losses = jnp.stack([top_loss, mid_loss, leaf_loss])
    return (query_grad, top_grad, mid_grad, leaf_grad, losses)


LANES = 128
SUB = 8
BF = jnp.bfloat16
F32 = jnp.float32
HIGH = lax.Precision.HIGHEST


def params(mib):
    return pltpu.CompilerParams(vmem_limit_bytes=mib * 1024 * 1024)


def iota(shape, dim):
    return lax.broadcasted_iota(jnp.int32, shape, dim)


def iota_f(shape, dim):
    return iota(shape, dim).astype(F32)


def dot_nn(a, b, precision=None):
    return lax.dot_general(
        a, b, (((1,), (0,)), ((), ())), precision=precision, preferred_element_type=F32
    )


def dot_nt(a, b, precision=None):
    return lax.dot_general(
        a, b, (((1,), (1,)), ((), ())), precision=precision, preferred_element_type=F32
    )


def dot_tn(a, b, precision=None):
    return lax.dot_general(
        a, b, (((0,), (0,)), ((), ())), precision=precision, preferred_element_type=F32
    )


def pack_kernel(
    q_ref, short_ref, slab_ref, leaf_t_ref, top_t_ref, pay_ref, info_ref, own_ref, *, devs, held
):
    rows, width = q_ref.shape
    short_len = short_ref.shape[0]
    clusters = slab_ref.shape[1]
    chunks = width // LANES
    slots = CAPB * held
    cluster_f = iota_f((rows, clusters), 1)
    slab = jnp.broadcast_to(slab_ref[...].astype(F32), (rows, clusters))
    short = short_ref[...].astype(F32)
    short = jnp.concatenate([short, jnp.zeros((rows - short_len, rows), F32)], axis=0).T
    places, hits = [], []
    for j in range(short_len):
        place = jnp.sum(jnp.where(short[:, j : j + 1] == cluster_f, slab, 0.0), axis=1, keepdims=True)
        places.append(place)
        hits.append(jnp.where(place == cluster_f, 1.0, 0.0))
    hit = functools.reduce(lambda a, b: a + b, hits)
    before = jnp.where(iota((rows, rows), 1) < iota((rows, rows), 0), 1.0, 0.0).astype(BF)
    count = dot_nn(before, hit.astype(BF))
    lane = iota((rows, LANES), 1)
    info = jnp.zeros((rows, LANES), F32)
    for j in range(short_len):
        rank = jnp.sum(hits[j] * count, axis=1, keepdims=True)
        info = jnp.where(lane == j, places[j], info)
        info = jnp.where(lane == short_len + j, rank, info)
    info_ref[...] = info
    queries = q_ref[...]
    own_ref[:rows, :] = queries
    top_target = jnp.broadcast_to(top_t_ref[...].astype(F32), (SUB, rows))
    high = jnp.floor(top_target * (1.0 / 256.0))
    code_at = iota((SUB, rows), 0)
    coded = jnp.where(code_at == 0, high, jnp.where(code_at == 1, top_target - 256.0 * high, 0.0))
    own_ref[rows:, :] = jnp.concatenate([coded] * chunks, axis=1).astype(BF)
    target = jnp.broadcast_to(leaf_t_ref[...].astype(F32) + 1.0, (SUB, rows)).astype(BF)
    ones = jnp.ones((SUB, rows), BF)
    table_rows = clusters // LANES
    table = jnp.zeros((CAPB * table_rows, LANES), F32)
    sub = iota((CAPB * table_rows, LANES), 0)
    for r in range(CAPB):
        pick = jnp.where(count == float(r), hit, 0.0)
        chosen = pick.astype(BF)
        first = (pick * hits[0]).astype(BF)
        code = dot_nn(ones, chosen) + dot_nn(target, first)
        for i in range(table_rows):
            part = jnp.broadcast_to(code[0:1, i * LANES : (i + 1) * LANES], table.shape)
            table = jnp.where(sub == r * table_rows + i, part, table)
        got = dot_tn(chosen, queries).astype(BF)
        for c in range(chunks):
            start = c * slots + r * held
            pay_ref[:, start : start + held, :] = got[:, c * LANES : (c + 1) * LANES].reshape(
                devs, held, LANES
            )
    coded = table.astype(BF)
    pay_ref[:, chunks * slots :, :] = jnp.broadcast_to(coded[None], (devs,) + coded.shape)


def halves(source, target, sems):
    half = source.shape[0] // 2
    return [
        pltpu.make_async_copy(
            source.at[pl.ds(n * half, half)], target.at[pl.ds(n * half, half)], sems.at[n]
        )
        for n in range(2)
    ]


def start(copies):
    for copy in copies:
        copy.start()
    return copies


def cluster_rows(wide_ref, k, devs, held, chunks):
    slots = CAPB * held
    return jnp.concatenate(
        [
            jnp.concatenate(
                [
                    wide_ref[pl.ds(c * slots + r * held + k, devs, stride=chunks * slots), :]
                    for c in range(chunks)
                ],
                axis=1,
            )
            for r in range(CAPB)
        ],
        axis=0,
    )


def forward_kernel(
    me_ref, got_ref, leaf_in, mid_ref, score_ref, stat_ref, code_ref,
    wide_ref, table_ref, leaf_ref, leaf_sem,
):
    devs, depth, _ = got_ref.shape
    held, labels, width = leaf_ref.shape
    fetches = start(halves(leaf_in, leaf_ref, leaf_sem))
    chunks = width // LANES
    slots = CAPB * held
    body = chunks * slots
    wide_ref[...] = got_ref[:, :body, :].reshape(devs * body, LANES).astype(F32)
    tail = depth - body
    table_ref[...] = got_ref[:, body:, :].astype(F32).reshape(devs * tail, LANES)
    first = me_ref[0] * held
    row_at = first // LANES
    lane_at = first - row_at * LANES
    lane = iota((devs, LANES), 1)
    codes = jnp.zeros((devs, LANES), F32)
    for r in range(CAPB):
        row = table_ref[pl.ds(r * (tail // CAPB) + row_at, devs, stride=tail), :]
        row = pltpu.roll(row, lax.rem(r * held - lane_at + LANES, LANES), 1)
        codes = jnp.where((lane >= r * held) & (lane < (r + 1) * held), row, codes)
    code_ref[...] = codes
    label_f = iota_f((CAPB * devs, labels), 1)
    stats = jnp.zeros((devs, LANES), F32)
    for k in range(held):
        full = cluster_rows(wide_ref, k, devs, held, chunks)
        rows = full.astype(BF)
        if k % (held // 2) == 0:
            fetches[k // (held // 2)].wait()
        scores = dot_nt(rows, leaf_ref[k])
        score_ref[k] = scores
        mid = jnp.sum(full * mid_ref[k : k + 1, :].astype(F32), axis=1, keepdims=True)
        peak = jnp.max(scores, axis=1, keepdims=True)
        lse = peak + jnp.log(jnp.sum(jnp.exp(scores - peak), axis=1, keepdims=True))
        code = jnp.concatenate(
            [codes[:, r * held + k : r * held + k + 1] for r in range(CAPB)], axis=0
        )
        target = jnp.sum(jnp.where(code - 2.0 == label_f, scores, 0.0), axis=1, keepdims=True)
        for n, value in enumerate((mid, lse, target)):
            for r in range(CAPB):
                stats = jnp.where(
                    lane == n * slots + r * held + k, value[r * devs : (r + 1) * devs], stats
                )
    stat_ref[...] = stats.reshape(stat_ref.shape)


def middle_kernel(info_ref, stat_ref, out_ref, loss_ref, *, devs, held, short_len):
    rows = info_ref.shape[0]
    slots = CAPB * held
    info = info_ref[...]
    stats = stat_ref[...].reshape(devs, LANES)
    lane = iota_f((rows, LANES), 1)
    dev_f = iota_f((rows, devs), 1)
    owners, spots, mids, lses = [], [], [], []
    for j in range(short_len):
        place = info[:, j : j + 1]
        rank = info[:, short_len + j : short_len + j + 1]
        dev = jnp.floor(place * (1.0 / held))
        spot = place - dev * held + rank * held
        owner = jnp.where(dev == dev_f, 1.0, 0.0)
        values = dot_nn(owner, stats, HIGH)
        owners.append(owner)
        spots.append(spot)
        mids.append(jnp.sum(jnp.where(lane == spot, values, 0.0), axis=1, keepdims=True))
        lses.append(jnp.sum(jnp.where(lane == spot + slots, values, 0.0), axis=1, keepdims=True))
        if j == 0:
            target = jnp.sum(
                jnp.where(lane == spot + 2 * slots, values, 0.0), axis=1, keepdims=True
            )

    def total(columns):
        peak = functools.reduce(jnp.maximum, columns)
        return peak + jnp.log(functools.reduce(lambda a, b: a + b, [jnp.exp(v - peak) for v in columns]))

    mid_total = total(mids)
    leaf_total = total(lses)
    back = []
    for j in range(short_len):
        delta = jnp.exp(mids[j] - mid_total) - (1.0 if j == 0 else 0.0)
        delta = delta.astype(BF).astype(F32)
        back.append(
            jnp.where(
                lane == spots[j], leaf_total, jnp.where(lane == spots[j] + slots, delta, 0.0)
            )
        )
    sent = dot_tn(jnp.concatenate(owners, axis=0), jnp.concatenate(back, axis=0), HIGH)
    out_ref[...] = sent.reshape(out_ref.shape)
    losses = jnp.where(lane == 0.0, mid_total - mids[0], jnp.where(lane == 1.0, leaf_total - target, 0.0))
    loss_ref[...] = losses.T[:SUB, :]


def slot_column(array, base, k, held):
    return jnp.concatenate(
        [array[:, base + r * held + k : base + r * held + k + 1] for r in range(CAPB)], axis=0
    )


def leaf_delta(scores, codes, norms, k, held):
    code = slot_column(codes, 0, k, held)
    onehot = jnp.where(code - 2.0 == iota_f(scores.shape, 1), 1.0, 0.0)
    chance = jnp.exp(scores - slot_column(norms, 0, k, held))
    return jnp.where(code > 0.5, chance - onehot, 0.0).astype(BF)


def backward_kernel(score_ref, code_ref, norm_ref, leaf_ref, mid_ref, pay_ref, wide_ref):
    held, pairs, _ = score_ref.shape
    devs = pairs // CAPB
    width = leaf_ref.shape[2]
    chunks = width // LANES
    slots = CAPB * held
    body = chunks * slots
    norms = norm_ref[...].reshape(devs, LANES)
    codes = code_ref[...]
    for k in range(held):
        delta = leaf_delta(score_ref[k], codes, norms, k, held)
        mid_delta = slot_column(norms, slots, k, held)
        back = dot_nn(delta, leaf_ref[k]) + mid_delta * mid_ref[k : k + 1, :].astype(F32)
        for r in range(CAPB):
            for c in range(chunks):
                wide_ref[pl.ds(c * slots + r * held + k, devs, stride=body), :] = back[
                    r * devs : (r + 1) * devs, c * LANES : (c + 1) * LANES
                ]
    pay_ref[...] = wide_ref[...].astype(BF).reshape(devs, body, LANES)


def grads_kernel(
    score_ref, code_ref, norm_ref, got_ref, leaf_grad_ref, mid_grad_ref, wide_ref
):
    held, pairs, _ = score_ref.shape
    devs = pairs // CAPB
    slots = CAPB * held
    chunks = leaf_grad_ref.shape[2] // LANES
    body = chunks * slots
    wide_ref[...] = got_ref[:, :body, :].reshape(devs * body, LANES).astype(F32)
    norms = norm_ref[...].reshape(devs, LANES)
    codes = code_ref[...]
    for k in range(held):
        full = cluster_rows(wide_ref, k, devs, held, chunks)
        delta = leaf_delta(score_ref[k], codes, norms, k, held)
        leaf_grad_ref[k] = dot_tn(delta, full.astype(BF))
        mid_delta = slot_column(norms, slots, k, held)
        mid_grad_ref[k : k + 1, :] = jnp.sum(mid_delta * full, axis=0, keepdims=True)


def finish_kernel(
    info_ref, back_ref, top_ref, top_loss_ref, pair_loss_ref, out_ref, loss_ref, *, held, short_len
):
    loss_ref[0:1, :] = top_loss_ref[0:1, :]
    loss_ref[1:3, :] = pair_loss_ref[0:2, :]
    rows, width = out_ref.shape
    devs = back_ref.shape[0]
    clusters = devs * held
    chunks = width // LANES
    slots = CAPB * held
    info = info_ref[...]
    cluster_f = iota_f((rows, clusters), 1)
    picks = []
    for r in range(CAPB):
        pick = jnp.zeros((rows, clusters), F32)
        for j in range(short_len):
            place = jnp.where(
                info[:, short_len + j : short_len + j + 1] == float(r), info[:, j : j + 1], -1.0
            )
            pick = jnp.where(place == cluster_f, 1.0, pick)
        picks.append(pick.astype(BF))
    for c in range(chunks):
        total = top_ref[:, c * LANES : (c + 1) * LANES]
        for r in range(CAPB):
            start = c * slots + r * held
            total = total + dot_nn(
                picks[r], back_ref[:, start : start + held, :].reshape(clusters, LANES)
            )
        out_ref[:, c * LANES : (c + 1) * LANES] = total


def top_step(block, target, pieces, weight_held, held_base):
    scores = jnp.concatenate([dot_nt(block, ref[...]) for ref in pieces], axis=1)
    peak = jnp.max(scores, axis=1, keepdims=True)
    total = peak + jnp.log(jnp.sum(jnp.exp(scores - peak), axis=1, keepdims=True))
    mine = dot_nt(block, weight_held)
    held_f = iota_f(mine.shape, 1) + held_base
    delta = (jnp.exp(mine - total) - jnp.where(target == held_f, 1.0, 0.0)).astype(BF)
    return scores, total, dot_tn(delta, block)


def top_column(codes):
    target = codes[0:1, :LANES].astype(F32) * 256.0 + codes[1:2, :LANES].astype(F32)
    return jnp.broadcast_to(target, (LANES, LANES)).T[:, 0:1]


def top_rows(blocks):
    rows = blocks[0].shape[0] - SUB
    block = jnp.concatenate([ref[:rows, :] for ref in blocks], axis=0)
    return block, jnp.concatenate([top_column(ref[rows:, :]) for ref in blocks], axis=0)


def own_columns(me, dims, label_size, held_top):
    steps = label_size // 2

    def split(value, size):
        high = jnp.floor((value + 0.5) * (1.0 / size))
        return high, value - high * size

    def flip(bit, other):
        return bit + other - 2.0 * bit * other

    dp_at, label_at = split(jnp.full(dims, me, jnp.int32).astype(F32), label_size)
    y_at, core_at = split(dp_at, 2)
    z_at, x_at = split(label_at, 2)
    part, rest = split(iota_f(dims, 1), 2 * held_top)
    side, row = split(rest, held_top)
    core_bit, y_bit = split(part, 2)
    dp_from = flip(y_at, y_bit) * 2.0 + flip(core_at, core_bit)
    z_from = z_at - dp_from - 1.0
    z_from = jnp.where(z_from < 0.0, z_from + steps, z_from)
    return (z_from * 2.0 + flip(x_at, side)) * held_top + row


def top_own_kernel(
    where_ref, me_ref, own_ref, blocks_ref, near_ref, y_ref, core_ref, far_ref, weight_ref,
    back_ref, part_ref, loss_ref, *, label_size,
):
    rows = own_ref.shape[0] - SUB
    piece = near_ref.shape[0]
    pieces = (near_ref, y_ref, core_ref, far_ref)
    blocks = [own_ref] + [blocks_ref.at[n] for n in range(blocks_ref.shape[0])]
    block, target = top_rows(blocks)
    scores, total, part = top_step(
        block, target, pieces, weight_ref[...], where_ref[0].astype(F32)
    )
    scores, total, target = scores[:rows], total[:rows], target[:rows]
    part_ref[...] = part
    column = own_columns(me_ref[0], (SUB, scores.shape[1]), label_size, weight_ref.shape[0])
    hit = jnp.broadcast_to(column[0:1, :], scores.shape) == target
    full = (jnp.exp(scores - total) - jnp.where(hit, 1.0, 0.0)).astype(BF)
    back = dot_nn(full[:, :piece], pieces[0][...])
    for n in range(1, len(pieces)):
        back = back + dot_nn(full[:, n * piece : (n + 1) * piece], pieces[n][...])
    back_ref[...] = back
    loss = total - jnp.sum(jnp.where(hit, scores, 0.0), axis=1, keepdims=True)
    loss_ref[...] = jnp.broadcast_to(loss, (rows, LANES)).T[:SUB, :]


def top_far_kernel(
    where_ref, me_ref, first_ref, blocks_ref, near_ref, y_ref, core_ref, far_ref, weight_ref, part_ref,
    kept_ref, given_ref, sum_ref, *, label_size,
):
    pieces = (near_ref, y_ref, core_ref, far_ref)
    blocks = [first_ref] + [blocks_ref.at[n] for n in range(blocks_ref.shape[0])]
    block, target = top_rows(blocks)
    base = where_ref[0].astype(F32)
    sum_ref[...] = part_ref[...] + top_step(block, target, pieces, weight_ref[...], base)[2]
    half = kept_ref.shape[0]
    core = lax.rem(lax.div(me_ref[0], label_size), 2)
    kept_ref[...] = sum_ref[pl.ds(pl.multiple_of(core * half, SUB), half), :]
    given_ref[...] = sum_ref[pl.ds(pl.multiple_of((1 - core) * half, SUB), half), :]


def spec():
    return pl.BlockSpec(memory_space=pltpu.VMEM)


def call(kernel, outs, ins, scratch=(), scalars=0, far_ins=(), far_outs=(), mib=58):
    far = pl.BlockSpec(memory_space=pltpu.HBM)
    small = pl.BlockSpec(memory_space=pltpu.SMEM)
    listed = isinstance(outs, tuple)
    out_specs = tuple(
        far if n in far_outs else spec() for n in range(len(outs) if listed else 1)
    )
    return pl.pallas_call(
        kernel,
        out_shape=outs,
        in_specs=[
            small if n < scalars else far if n in far_ins else spec() for n in range(len(ins))
        ],
        out_specs=out_specs if listed else out_specs[0],
        scratch_shapes=list(scratch),
        compiler_params=params(mib),
    )(*ins)


def shape(dims, dtype):
    return jax.ShapeDtypeStruct(dims, dtype)


def fits(queries, leaf_weight, shortlist, top_weight, devs, dp_size, label_size):
    rows, width = queries.shape
    held, labels = leaf_weight.shape[:2]
    return (
        rows == LANES
        and labels == LANES
        and width % LANES == 0
        and held % 16 == 0
        and LANES % held == 0
        and 3 * CAPB * held <= LANES
        and CAPB * (devs * held // LANES) % SUB == 0
        and devs % SUB == 0
        and dp_size == 4
        and label_size == 2 * dp_size
        and top_weight.shape[0] % 32 == 0
        and top_weight.shape[0] * label_size <= 65536
        and 2 * shortlist.shape[1] <= LANES
    )


def after(value, first):
    return lax.optimization_barrier((value, first))[0]


def exchange(array):
    return lax.all_to_all(array, ("dp", "label"), split_axis=0, concat_axis=0, tiled=True)


def per_device(
    queries, shortlist, slab_slot, top_target, leaf_target, top_weight, mid_weight, leaf_weight
):
    dp_size = lax.axis_size("dp")
    label_size = lax.axis_size("label")
    devs = dp_size * label_size
    if not fits(queries, leaf_weight, shortlist, top_weight, devs, dp_size, label_size):
        return per_device_any(
            queries, shortlist, slab_slot, top_target, leaf_target, top_weight, mid_weight, leaf_weight
        )
    rows, width = queries.shape
    held, labels = leaf_weight.shape[:2]
    short_len = shortlist.shape[1]
    clusters = devs * held
    chunks = width // LANES
    slots = CAPB * held
    body = chunks * slots
    tail = CAPB * clusters // LANES
    dp_at = lax.axis_index("dp")
    label_at = lax.axis_index("label")
    me = dp_at * label_size + label_at

    steps = label_size // 2
    held_top = top_weight.shape[0]
    flip_x = [(i, i ^ 1) for i in range(label_size)]
    flip_y = [(i, i ^ 2) for i in range(dp_size)]
    flip_core = [(i, i ^ 1) for i in range(dp_size)]

    def along(step):
        return [
            (z * 2 + x, ((z - step) % steps) * 2 + x) for z in range(steps) for x in range(2)
        ]

    shift_z = [
        (d * label_size + z * 2 + x, d * label_size + (z + d + 1) % steps * 2 + x)
        for d in range(dp_size)
        for z in range(steps)
        for x in range(2)
    ]
    w_near = lax.ppermute(top_weight, ("dp", "label"), shift_z)
    me = me.astype(jnp.int32)[None]
    label_base = (label_at * held_top).astype(jnp.int32)[None]
    payload, info, own = call(
        functools.partial(pack_kernel, devs=devs, held=held),
        (
            shape((devs, body + tail, LANES), BF),
            shape((rows, LANES), F32),
            shape((rows + SUB, width), BF),
        ),
        (
            after(queries, (me, label_base)),
            shortlist.T,
            slab_slot[None, :],
            leaf_target[None, :],
            top_target[None, :],
        ),
    )
    got = exchange(payload)
    w_other = lax.ppermute(w_near, "label", flip_x)
    w_own = jnp.concatenate([w_near, w_other])
    w_y = lax.ppermute(w_own, "dp", flip_y)
    w_core = lax.ppermute(w_own, "dp", flip_core)
    sent = after(own, w_near)
    own_other = lax.ppermute(own, "label", flip_x)
    peers = [lax.ppermute(sent, "label", along(n)) for n in range(1, steps)]
    pairs = CAPB * devs
    scores, stats, codes = call(
        forward_kernel,
        (
            shape((held, pairs, labels), F32),
            shape((devs, 1, LANES), F32),
            shape((devs, LANES), F32),
        ),
        (me, got, leaf_weight, mid_weight),
        scratch=(
            pltpu.VMEM((devs * body, LANES), F32),
            pltpu.VMEM((devs * tail, LANES), F32),
            pltpu.VMEM((held, labels, width), BF),
            pltpu.SemaphoreType.DMA((2,)),
        ),
        scalars=1,
        far_ins=(2,),
        mib=50,
    )
    w_y = after(w_y, stats)
    w_far = lax.ppermute(w_y, "dp", flip_core)
    stats_back = exchange(stats)
    norms, pair_losses = call(
        functools.partial(middle_kernel, devs=devs, held=held, short_len=short_len),
        (shape((devs, 1, LANES), F32), shape((SUB, rows), F32)),
        (info, stats_back),
        mib=16,
    )
    norms_held = exchange(norms)
    mine = jnp.stack(after(peers, norms))
    other = lax.ppermute(mine, "label", flip_x)
    back = call(
        backward_kernel,
        shape((devs, body, LANES), BF),
        (scores, codes, norms_held, leaf_weight, mid_weight),
        scratch=(pltpu.VMEM((devs * body, LANES), F32),),
        mib=24,
    )
    returned = exchange(back)
    top_back, top_part, top_loss = call(
        functools.partial(top_own_kernel, label_size=label_size),
        (
            shape((rows, width), F32),
            shape((held_top, width), F32),
            shape((SUB, rows), F32),
        ),
        (label_base, me, own, after(mine, back), w_own, w_y, w_core, w_far, top_weight),
        scalars=2,
    )
    kept, given = call(
        functools.partial(top_far_kernel, label_size=label_size),
        (shape((held_top // 2, width), F32), shape((held_top // 2, width), F32)),
        (label_base, me, own_other, after(other, back), w_own, w_y, w_core, w_far, top_weight, top_part),
        scalars=2,
        scratch=(pltpu.VMEM((held_top, width), F32),),
    )
    core = dp_at % 2
    share = kept + lax.ppermute(given, "dp", flip_core)
    from_y = lax.ppermute(share, "dp", flip_y)
    leaf_grad, mid_grad = call(
        grads_kernel,
        (shape((held, labels, width), F32), shape((held, width), F32)),
        (scores, codes, norms_held, after(got, share)),
        scratch=(pltpu.VMEM((devs * body, LANES), F32),),
    )
    share = share + after(from_y, mid_grad)
    rest = lax.ppermute(share, "dp", flip_core)
    top_grad = jnp.concatenate(
        [jnp.where(core == 0, share, rest), jnp.where(core == 0, rest, share)]
    )
    query_grad, losses = call(
        functools.partial(finish_kernel, held=held, short_len=short_len),
        (shape((rows, width), F32), shape((3, rows), F32)),
        (info, returned, top_back, top_loss, pair_losses),
        mib=16,
    )
    return (query_grad, top_grad, mid_grad, leaf_grad, losses)


def solution(mesh):
    in_specs = (
        P(("dp", "label"), None),
        P(("dp", "label"), None),
        P(),
        P(("dp", "label")),
        P(("dp", "label")),
        P("label", None),
        P(("dp", "label"), None),
        P(("dp", "label"), None, None),
    )
    out_specs = (
        P(("dp", "label"), None),
        P("label", None),
        P(("dp", "label"), None),
        P(("dp", "label"), None, None),
        P(None, ("dp", "label")),
    )
    return jax.shard_map(
        per_device, mesh=mesh, in_specs=in_specs, out_specs=out_specs, check_vma=False
    )
```
